32 devices in a mesh: dp: 2 (over x), expert: 8 (over z, core), tensor: 2 (over y).
Axes of the slice: x: 2, y: 2, z: 4, core: 2. Of those that a mesh axis runs over, the one named last changes fastest.
Arguments:
- tokens: bfloat16 [192, 256, 1280], P(('dp', 'expert', 'tensor')), may hold values from -16 to 16
- cotangent: bfloat16 [192, 256, 1280], P(('dp', 'expert', 'tensor')), may hold values from -6 to 6
- norm_gain: float32 [1280], replicated, may hold values from 0.5 to 1.5
- slot_keys: bfloat16 [1280, 16], replicated, may hold values from -2 to 2
- w_in: bfloat16 [8, 1280, 2560], P('expert', None, 'tensor'), may hold values from -0.15625 to 0.15625
- w_out: bfloat16 [8, 2560, 1280], P('expert', 'tensor'), may hold values from -0.125 to 0.125
Outputs:
- grad_tokens: bfloat16 [192, 256, 1280], P(('dp', 'expert', 'tensor'))
- grad_gain: float32 [1280], replicated
- grad_keys: float32 [1280, 16], replicated
- grad_in: bfloat16 [8, 1280, 2560], P('expert', 'dp', 'tensor')
- grad_out: bfloat16 [8, 2560, 1280], P('expert', 'tensor', 'dp')
The draws below stay inside these ranges and needn't reach their ends.
All inputs are finite; a program needn't handle non-finite values.
Results may differ from the reference program's by a relative error of at most 0.014.
The reference program's roundings to bfloat16 on the way count: a program that leaves them out, or rounds other values in their place, can miss the bound.
Values may be sent and summed in bfloat16 or wider, within the bound.
A program may use at most 128 MiB of HBM per device.

```python
import math
import jax
import jax.numpy as jnp
from jax import lax

D = 1280
TOK_IMG = 256
SLOT_PER = 2
FF = 2560
IMG_DEV = 6
EXPERTS = 8
SLOTS = 16
IMAGES = 192


def draw_slot_keys(key, part):
    values = jax.random.normal(jax.random.fold_in(key, 11), (D, SLOTS), jnp.float32) * (1.0 / math.sqrt(D))
    limit = 1.0 + 2000 // D
    return jnp.clip(values, -limit, limit).astype(jnp.bfloat16)


def draw_tokens(key, part):
    values = jax.random.normal(jax.random.fold_in(key, 21), (IMAGES, TOK_IMG, D), jnp.float32)
    return jnp.clip(values, -16.0, 16.0).astype(jnp.bfloat16)


def level_of(rng, shape, split, smallest, largest):
    factor_of = 1.0
    for dim, blocks in split:
        draws = jax.random.uniform(jax.random.fold_in(jax.random.fold_in(rng, 6), dim), (blocks,), jnp.float32, smallest / len(split), largest / len(split))
        factor_of = factor_of * jnp.repeat(jnp.exp(draws), shape[dim] // blocks).reshape((-1,) + (1,) * (len(shape) - 1 - dim))
    return factor_of


def bell_draw(rng, extent, scale, most, split=(), dtype=jnp.bfloat16):
    values = scale * jax.random.normal(rng, extent, jnp.float32)
    if split:
        values = values * level_of(rng, extent, split, -0.22, 0.18)
    return jnp.clip(values, -most, most).astype(dtype)


def setup_inputs(seed: int = 0) -> dict:
    arg_keys = jax.random.split(jax.random.key(seed), 7)
    tokens = draw_tokens(jax.random.fold_in(arg_keys[6], 71), 0)
    cotangent = bell_draw(arg_keys[1], (IMAGES, TOK_IMG, D), 1.0, 6.0, ((0, 32),))
    norm_gain = jnp.clip(1.0 + 0.1 * jax.random.normal(arg_keys[2], (D,), jnp.float32), 0.5, 1.5)
    slot_keys = draw_slot_keys(jax.random.fold_in(arg_keys[6], 71), 0)
    w_in = bell_draw(arg_keys[4], (EXPERTS, D, FF), D ** -0.5, 0.15625, ((0, 8), (2, 2)))
    w_out = bell_draw(arg_keys[5], (EXPERTS, FF, D), FF ** -0.5, 0.125, ((0, 8), (1, 2)))
    return dict(tokens=tokens, cotangent=cotangent, norm_gain=norm_gain, slot_keys=slot_keys, w_in=w_in, w_out=w_out)


EPSILON = 1e-06

def rounded(values):
    lowered = lax.optimization_barrier(values.astype(jnp.bfloat16))
    return values + lax.stop_gradient(lowered.astype(jnp.float32) - values)

def mixing(tokens_wide, gain, keys_wide):
    average = lax.optimization_barrier(jnp.mean(tokens_wide, axis=-1, keepdims=True))
    centred = tokens_wide - average
    spread = lax.optimization_barrier(jnp.mean(centred * centred, axis=-1, keepdims=True))
    normed = rounded(centred * lax.rsqrt(spread + EPSILON) * gain)
    logits = jnp.einsum('bmd,dn->bmn', normed, keys_wide, precision=lax.Precision.HIGHEST)
    dispatch = rounded(jax.nn.softmax(logits, axis=1))
    combine = jax.nn.softmax(logits, axis=2)
    slot_values = jnp.einsum('bmn,bmd->bnd', dispatch, normed, precision=lax.Precision.HIGHEST)
    return (slot_values, combine)

def expert_forward(slot_rows, first_proj, second_proj):
    pre_act = jnp.dot(slot_rows.astype(jnp.float32), first_proj.astype(jnp.float32), preferred_element_type=jnp.float32)
    hidden = jax.nn.gelu(pre_act).astype(jnp.bfloat16)
    return jnp.dot(hidden.astype(jnp.float32), second_proj.astype(jnp.float32), preferred_element_type=jnp.float32).astype(jnp.bfloat16)

def expert_backward(slot_rows, row_grads, first_proj, second_proj):
    pre_act = jnp.dot(slot_rows.astype(jnp.float32), first_proj.astype(jnp.float32), preferred_element_type=jnp.float32)
    hidden = jax.nn.gelu(pre_act).astype(jnp.bfloat16)
    grad_hidden = lax.dot_general(row_grads.astype(jnp.float32), second_proj.astype(jnp.float32), (((1,), (1,)), ((), ())), preferred_element_type=jnp.float32)
    grad_pre = jax.vjp(jax.nn.gelu, pre_act)[1](grad_hidden)[0].astype(jnp.bfloat16)
    grad_rows = lax.dot_general(grad_pre.astype(jnp.float32), first_proj.astype(jnp.float32), (((1,), (1,)), ((), ())), preferred_element_type=jnp.float32)
    grad_first = lax.dot_general(slot_rows.astype(jnp.float32), grad_pre.astype(jnp.float32), (((0,), (0,)), ((), ())), preferred_element_type=jnp.float32)
    grad_second = lax.dot_general(hidden.astype(jnp.float32), row_grads.astype(jnp.float32), (((0,), (0,)), ((), ())), preferred_element_type=jnp.float32)
    return (grad_rows.astype(jnp.bfloat16), grad_first.astype(jnp.bfloat16), grad_second.astype(jnp.bfloat16))

def to_experts(per_image, images):
    experts = SLOTS // SLOT_PER
    shaped = per_image.reshape(images, experts, SLOT_PER, D)
    return jnp.transpose(shaped, (1, 0, 2, 3)).reshape(experts, images * SLOT_PER, D)

def from_experts(per_expert, images):
    experts = SLOTS // SLOT_PER
    shaped = per_expert.reshape(experts, images, SLOT_PER, D)
    return jnp.transpose(shaped, (1, 0, 2, 3)).reshape(images // IMG_DEV, IMG_DEV, SLOTS, D)

def reference(tokens, cotangent, norm_gain, slot_keys, w_in, w_out):
    images = tokens.shape[0]
    groups = images // IMG_DEV
    image_blocks = tokens.reshape(groups, IMG_DEV, TOK_IMG, D)
    grad_blocks = cotangent.reshape(groups, IMG_DEV, TOK_IMG, D)
    keys_wide = slot_keys.astype(jnp.float32)

    def forward_block(image_block):
        slot_values, combine = mixing(image_block.astype(jnp.float32), norm_gain, keys_wide)
        return (slot_values.astype(jnp.bfloat16), combine.astype(jnp.bfloat16))
    slot_inputs, combine_low = lax.map(forward_block, image_blocks)
    expert_rows = to_experts(slot_inputs, images)
    slot_outputs = lax.map(lambda inputs: expert_forward(inputs[0], inputs[1], inputs[2]), (expert_rows, w_in, w_out))
    slot_outputs = from_experts(slot_outputs, images)

    def combine_block(inputs):
        comb_block, grad_block, out_block = inputs
        grad_slots = jnp.einsum('bmn,bmd->bnd', comb_block.astype(jnp.float32), grad_block.astype(jnp.float32))
        grad_combine = jnp.einsum('bmd,bnd->bmn', grad_block.astype(jnp.float32), out_block.astype(jnp.float32))
        return (grad_slots.astype(jnp.bfloat16), grad_combine)
    grad_slots, grad_combine = lax.map(combine_block, (combine_low, grad_blocks, slot_outputs))
    grad_rows_in = to_experts(grad_slots, images)
    grad_rows, grad_first, grad_second = lax.map(lambda inputs: expert_backward(inputs[0], inputs[1], inputs[2], inputs[3]), (expert_rows, grad_rows_in, w_in, w_out))
    grad_slot_in = from_experts(grad_rows, images)

    def mixing_back(totals, inputs):
        image_block, grad_block, slot_grad, comb_grad = inputs
        unused, pullback = jax.vjp(mixing, image_block.astype(jnp.float32), norm_gain, keys_wide)
        grad_tok, grad_gain, grad_keys = pullback((slot_grad.astype(jnp.float32), comb_grad))
        result = (grad_block.astype(jnp.float32) + grad_tok).astype(jnp.bfloat16)
        return ((totals[0] + grad_gain, totals[1] + grad_keys), result)
    start_totals = (jnp.zeros((D,), jnp.float32), jnp.zeros((D, SLOTS), jnp.float32))
    totals, grad_tokens = lax.scan(mixing_back, start_totals, (image_blocks, grad_blocks, grad_slot_in, grad_combine))
    return (grad_tokens.reshape(images, TOK_IMG, D), totals[0], totals[1], grad_first, grad_second)
```

```python
import functools
import types

import jax
import jax.numpy as jnp
import numpy as np
from jax import lax
from jax.experimental import pallas as pl
from jax.experimental.pallas import tpu as pltpu
from jax.sharding import PartitionSpec as P

AXES = ("dp", "expert", "tensor")
MESH = pl.DeviceIdType.MESH
SLOT_PER = 2
EPSILON = 1e-06
GELU_A = 0.7978845608028654
GELU_B = 0.044715
TILE = 256
ROWS = 64
LOW, WIDE = jnp.bfloat16, jnp.float32


def contract_rows(left, right):
    return lax.dot_general(left, right, (((0,), (0,)), ((), ())), preferred_element_type=WIDE)


def contract_cols(left, right):
    return lax.dot_general(left, right, (((1,), (1,)), ((), ())), preferred_element_type=WIDE)


def gelu_of(x):
    return 0.5 * x * (1.0 + jnp.tanh(GELU_A * (x + GELU_B * (x * x * x))))


def gelu_slope(x):
    square = x * x
    bend = jnp.tanh(GELU_A * (x + GELU_B * (square * x)))
    return 0.5 * (1.0 + bend) + 0.5 * x * (1.0 - bend * bend) * (
        GELU_A * (1.0 + 3.0 * GELU_B * square)
    )


def around(position, step, size):
    return lax.rem(position + (step + size), size)


def tables(pair, experts, tensor):
    slots, quarter = experts * SLOT_PER, pair * SLOT_PER
    height, own = 2 * quarter, experts * quarter
    group = tensor * own

    def hot(source):
        table = np.zeros((source.size, source.size), np.float32)
        table[np.arange(source.size), source] = 1.0
        return jnp.asarray(table, LOW)

    r = np.arange(experts * height)
    e, stream, u = r // height, r % height // quarter, r % quarter
    image_order = stream * pair * slots + u // SLOT_PER * slots + e * SLOT_PER + u % SLOT_PER
    stream_order = stream * own + e * quarter + u
    r = np.arange(2 * group)
    block_order = r % group // quarter * height + r // group * quarter + r % quarter
    r = np.arange(experts * height)
    image, stream, slot = r // (2 * slots), r % (2 * slots) // slots, r % slots
    back_order = slot // SLOT_PER * height + stream * quarter + image * SLOT_PER + slot % SLOT_PER
    return hot(image_order), hot(block_order), hot(stream_order), hot(back_order)


def exchange_kernel(sizes, spread, names, *refs):
    dp, experts, tensor = sizes
    r = types.SimpleNamespace(**dict(zip(names, refs)))
    d, e, t = (lax.axis_index(name) for name in AXES)
    images, count, features = r.x.shape
    slots, units = r.keys.shape[0], r.w1.shape[1]
    chunks, _, height, _ = r.blk.shape
    pair, quarter = images // chunks, height // 2
    own = experts * quarter
    group = tensor * own
    lanes = features // 128
    mine = d if spread > 1 else 0
    where = [d, e, t]

    def push(src, dst, send, recv, axis, place):
        target = {"dp": d, "expert": e, "tensor": t}
        target[axis] = place
        return pltpu.make_async_remote_copy(
            src_ref=src, dst_ref=dst, send_sem=send, recv_sem=recv,
            device_id=tuple(target[name] for name in AXES), device_id_type=MESH,
        )

    started = []

    def launch(copy):
        copy.start()
        started.append(copy)

    offsets = [(a, b, c) for a in range(dp) for b in range(experts) for c in range(tensor)]
    targets = [tuple(around(w, k, s) for w, k, s in zip(where, step, sizes)) for step in offsets]
    sources = [tuple(around(w, -k, s) for w, k, s in zip(where, step, sizes)) for step in offsets]
    others = range(1, len(offsets))
    rank = lambda p: (p[0] * experts + p[1]) * tensor + p[2]

    fetched = []

    def fetch(src, dst):
        copy = pltpu.make_async_copy(src, dst, r.in_sem.at[len(fetched)])
        copy.start()
        fetched.append(copy)
        return copy

    def image_copy(b, n):
        return pltpu.make_async_copy(
            (r.x_in, r.c_in)[n].at[b], (r.x, r.c)[n].at[b], r.image_sem.at[n, b])

    image_copy(0, 0).start()
    small = [fetch(r.gain_in, r.gain_rows), fetch(r.keys_in, r.keys), fetch(r.mixes_in, r.mixes)]
    image_copy(0, 1).start()
    barrier = pltpu.get_barrier_semaphore()
    for k in others:
        pl.semaphore_signal(barrier, inc=1, device_id=targets[k], device_id_type=MESH)
    for b in range(1, images):
        image_copy(b, 0).start()
        image_copy(b, 1).start()
    unp_copy, ret_copy, sel_copy = (
        fetch(r.unp_in, r.unp), fetch(r.ret_in, r.turn), fetch(r.sel_in, r.sel))
    w1_copy, w2_copy = fetch(r.w1_in, r.w1), fetch(r.w2_in, r.w2)
    for copy in small:
        copy.wait()
    r.gains[...] = jnp.concatenate([r.gain_rows[n:n + 1, :] for n in range(lanes)], axis=1)
    r.keys_sum[...] = jnp.zeros_like(r.keys_sum)
    r.gain_sum[...] = jnp.zeros_like(r.gain_sum)

    def mix_image(b, slab):
        image_copy(b, 0).wait()
        gains = r.gains[...]

        def rows_of(n, carry):
            rows = pl.ds(pl.multiple_of(n * ROWS, ROWS), ROWS)
            values = r.x[b, rows, :].astype(WIDE)
            average = jnp.mean(values, axis=-1, keepdims=True)
            centred = values - average
            inverse = lax.rsqrt(jnp.mean(centred * centred, axis=-1, keepdims=True) + EPSILON)
            r.normed[b, rows, :] = (centred * inverse * gains).astype(LOW)
            lane = lax.broadcasted_iota(jnp.int32, (ROWS, 128), 1)
            r.stat[b, rows, :] = jnp.where(lane == 0, average, inverse)
            return carry

        lax.fori_loop(0, count // ROWS, rows_of, 0)
        logits = contract_cols(r.keys[...], r.normed[b])
        over_tokens = jnp.exp(logits - jnp.max(logits, axis=1, keepdims=True))
        over_tokens = over_tokens / jnp.sum(over_tokens, axis=1, keepdims=True)
        over_slots = jnp.exp(logits - jnp.max(logits, axis=0, keepdims=True))
        over_slots = over_slots / jnp.sum(over_slots, axis=0, keepdims=True)
        r.logits[b] = logits
        r.disp[b] = over_tokens
        r.comb[b] = over_slots
        image_copy(b, 1).wait()
        taken = jnp.dot(over_tokens.astype(LOW), r.normed[b], preferred_element_type=WIDE)
        given = jnp.dot(over_slots.astype(LOW), r.c[b], preferred_element_type=WIDE)
        r.slot_in[b] = taken
        start = pl.multiple_of(slab * slots, slots)
        r.stack[pl.ds(start, slots), :] = taken.astype(LOW)
        start = pl.multiple_of((pair + slab) * slots, slots)
        r.stack[pl.ds(start, slots), :] = given.astype(LOW)

    def mix(c):
        @pl.loop(0, pair)
        def _(slab):
            mix_image(c * pair + slab, slab)

        moved = jnp.dot(r.mixes[...], r.stack[...], preferred_element_type=WIDE)
        for n in range(experts):
            r.blk[c, n] = moved[n * height:(n + 1) * height].astype(LOW)

    near = sorted(range(1, experts), key=lambda k: -min(k, experts - k))
    arrive = {}

    def scatter(c):
        for k in near:
            to = around(e, k, experts)
            arrive[c, k] = push(r.blk.at[c, to], r.rows.at[c, mine, t, e],
                                r.zs.at[c, k], r.zr.at[c, k], "expert", to)
            launch(arrive[c, k])
        share_rows(c, r.blk.at[c, e], 0)
        r.rows[c, mine, t, e] = r.blk[c, e]

    def share_rows(c, src, k):
        slot = r.rows.at[c, mine, t, around(e, -k, experts)]
        for j in range(1, tensor):
            launch(push(src, slot, r.ys.at[c, j, k], r.yr.at[c, j, k], "tensor", around(t, j, tensor)))

    def share_slab(c, j):
        for i in range(1, spread):
            slab = r.rows.at[c, mine, around(t, -j, tensor)]
            launch(push(slab, slab, r.xs.at[c, j, i], r.xr.at[c, j, i], "dp", around(d, i, dp)))

    def forward_rows(c):
        for k in near:
            arrive[c, k].wait_recv()
            share_rows(c, r.rows.at[c, mine, t, around(e, -k, experts)], k)
        share_slab(c, 0)

    def gather_rows(c):
        for j in range(1, tensor):
            for k in [0] + near:
                slot = r.rows.at[c, mine, around(t, -j, tensor), around(e, -k, experts)]
                push(slot, slot, r.ys.at[c, j, k], r.yr.at[c, j, k],
                     "tensor", around(t, j, tensor)).wait_recv()
            share_slab(c, j)

    def unpack(c, place, base):
        block = r.rows[c, place].reshape(2 * group, features)
        both = jnp.dot(r.unp[...], block, preferred_element_type=WIDE)
        r.s_all[pl.ds(base, group), :] = both[0:group].astype(LOW)
        r.g_all[pl.ds(base, group), :] = both[group:].astype(LOW)

    def tiles(extent):
        def over(body):
            @pl.loop(0, extent // TILE)
            def _(n):
                body(pl.ds(pl.multiple_of(n * TILE, TILE), TILE))
        return over

    def forward(base, size):
        @tiles(units)
        def _(cols):
            x = jnp.dot(r.s_all[pl.ds(base, size), :], r.w1[:, cols], preferred_element_type=WIDE)
            r.pre[pl.ds(0, size), cols] = x
            r.h_all[pl.ds(base, size), cols] = gelu_of(x).astype(LOW)

    def backward(base, size):
        @tiles(units)
        def _(cols):
            x = contract_cols(r.g_all[pl.ds(base, size), :], r.w2[cols, :])
            r.p_all[pl.ds(base, size), cols] = (x * gelu_slope(r.pre[pl.ds(0, size), cols])).astype(LOW)

    def project(c, base):
        @tiles(features)
        def _(cols):
            r.part[c, 0, :, cols] = jnp.dot(
                r.h_all[pl.ds(base, group), :], r.w2[:, cols], preferred_element_type=WIDE)

        share_part(c, 0)

    def project_back(c, base):
        @tiles(features)
        def _(cols):
            r.part[c, 1, :, cols] = contract_cols(r.p_all[pl.ds(base, group), :], r.w1[cols, :])

        share_part(c, 1)

    def part_copy(c, which, j):
        return push(r.sent.at[c, which, j - 1], r.got.at[c, which, j - 1],
                    r.ps.at[c, which, j], r.pr.at[c, which, j], "tensor", around(t, j, tensor))

    def share_part(c, which):
        for j in range(1, tensor):
            to = around(t, j, tensor)
            r.sent[c, which, j - 1] = r.part[c, which, pl.ds(pl.multiple_of(to * own, 8), own), :].astype(LOW)
            launch(part_copy(c, which, j))

    def give_back(c):
        totals = []
        for which in range(2):
            total = r.part[c, which, pl.ds(pl.multiple_of(t * own, 8), own), :]
            for j in range(1, tensor):
                part_copy(c, which, j).wait_recv()
                total = total + r.got[c, which, j - 1].astype(WIDE)
            totals.append(total.astype(LOW))
        moved = jnp.dot(r.turn[...], jnp.concatenate(totals, axis=0), preferred_element_type=WIDE)
        for n in range(experts):
            r.ret[c, n] = moved[n * height:(n + 1) * height].astype(LOW)
        for k in near:
            to = around(e, k, experts)
            arrive["back", c, k] = push(r.ret.at[c, to], r.back.at[c, e],
                                        r.bs.at[c, k], r.br.at[c, k], "expert", to)
            launch(arrive["back", c, k])
        r.back[c, e] = r.ret[c, e]

    def image_gradients(b, slab):
        start = pl.multiple_of(slab * 2 * slots, 2 * slots)
        returned = r.found[pl.ds(start, slots), :]
        slot_grad = r.found[pl.ds(start + slots, slots), :]
        grad_dispatch = contract_cols(slot_grad, r.normed[b])
        grad_combine = contract_cols(returned, r.c[b])
        dispatch, combine = r.disp[b], r.comb[b]
        logit = dispatch * (
            grad_dispatch - jnp.sum(dispatch * grad_dispatch, axis=1, keepdims=True)
        ) + combine * (grad_combine - jnp.sum(combine * grad_combine, axis=0, keepdims=True))
        first = logit.astype(LOW)
        rest = logit - first.astype(WIDE)
        second = rest.astype(LOW)
        third = (rest - second.astype(WIDE)).astype(LOW)
        low = dispatch.astype(LOW)
        split = jnp.concatenate([first, second, third], axis=0)
        r.left[b, 0:slots, :] = low
        r.left[b, slots:4 * slots, :] = split
        r.right[b] = slot_grad
        parts = jnp.dot(split, r.normed[b], preferred_element_type=WIDE)
        r.keys_sum[...] += parts[0:slots] + parts[slots:2 * slots] + parts[2 * slots:3 * slots]
        wide = slot_grad.astype(WIDE)
        r.gain_sum[...] += wide * r.slot_in[b]
        low = low.astype(WIDE)
        gains = r.gains[...]
        from_slots = jnp.sum(wide * gains, axis=1, keepdims=True)
        from_keys = jnp.sum(r.keys[...].astype(WIDE) * gains, axis=1, keepdims=True)
        first_mean = jnp.sum(low * from_slots + logit * from_keys, axis=0, keepdims=True)
        second_mean = jnp.sum(low * grad_dispatch + logit * r.logits[b], axis=0, keepdims=True)
        row = lax.broadcasted_iota(jnp.int32, (8, count), 0)
        r.moment[b] = jnp.where(row == 0, first_mean, second_mean) * (1.0 / features)

    def take_back(c):
        for k in near:
            arrive["back", c, k].wait_recv()
        block = r.back[c].reshape(experts * height, features)
        r.found[...] = jnp.dot(r.sel[...], block, preferred_element_type=WIDE).astype(LOW)

        @pl.loop(0, pair)
        def _(slab):
            image_gradients(c * pair + slab, slab)

    placed = []

    def place_out(src, dst):
        copy = pltpu.make_async_copy(src, dst, r.out_sem.at[len(placed)])
        copy.start()
        placed.append(copy)

    for c in range(chunks):
        mix(c)
        if c == 0:
            pl.semaphore_wait(barrier, len(others))
        scatter(c)
    for copy in (unp_copy, ret_copy, sel_copy, w1_copy, w2_copy):
        copy.wait()
    place_out(r.stat, r.stat_out)
    forward_rows(0)
    for c in range(chunks):
        base = c * group
        gather_rows(c)
        unpack(c, mine, base)
        forward(base, group)
        if c > 0:
            give_back(c - 1)
        project(c, base)
        backward(base, group)
        if c + 1 < chunks:
            forward_rows(c + 1)
        project_back(c, base)
    full = chunks * group

    def other_rows(i):
        other = around(d, -i, dp)
        for c in range(chunks):
            for j in range(tensor):
                slab = r.rows.at[c, other, around(t, -j, tensor)]
                push(slab, slab, r.xs.at[c, j, i], r.xr.at[c, j, i], "dp", around(d, i, dp)).wait_recv()
            unpack(c, other, i * full + c * group)

    for i in range(1, spread):
        other_rows(i)
        forward(i * full, full)
    give_back(chunks - 1)
    for i in range(1, spread):
        backward(i * full, full)
    if r.s_out.shape[1] != features:
        part_cols = pl.ds(pl.multiple_of(d * r.s_out.shape[1], 128), r.s_out.shape[1])
    else:
        part_cols = slice(None)
    place_out(r.s_all.at[:, part_cols], r.s_out)
    place_out(r.g_all.at[:, part_cols], r.g_out)
    place_out(r.h_all, r.h_out)
    place_out(r.p_all, r.p_out)
    for c in range(chunks):
        take_back(c)
    place_out(r.left, r.left_out)
    place_out(r.right, r.right_out)
    place_out(r.moment, r.moment_out)

    each = r.pack.shape[1] // 8
    bands = slots // 8
    count_tiles = bands * lanes + -(-lanes // 8)
    owners = -(-count_tiles // each)
    me = rank(where)
    gain = jnp.sum(r.gain_sum[...] + r.keys[...].astype(WIDE) * r.keys_sum[...], axis=0, keepdims=True)
    gain = gain / r.gains[...]
    for n in range(bands * lanes):
        band, lane = n // lanes, n % lanes
        r.pack[n // each, pl.ds(n % each * 8, 8), :] = r.keys_sum[
            band * 8:band * 8 + 8, lane * 128:lane * 128 + 128]
    for n in range(-(-lanes // 8) * 8):
        m = bands * lanes + n // 8
        row = m % each * 8 + n % 8
        piece = gain[:, n * 128:n * 128 + 128] if n < lanes else jnp.zeros((1, 128), WIDE)
        r.pack[m // each, row:row + 1, :] = piece

    def reduce_copy(k):
        return pltpu.make_async_remote_copy(
            src_ref=r.pack.at[rank(targets[k])], dst_ref=r.heap.at[k], send_sem=r.ss.at[k],
            recv_sem=r.sr.at[k], device_id=targets[k], device_id_type=MESH)

    def spread_copy(k):
        return pltpu.make_async_remote_copy(
            src_ref=r.total, dst_ref=r.summed.at[me], send_sem=r.gs.at[k],
            recv_sem=r.gr.at[k], device_id=targets[k], device_id_type=MESH)

    def gated(test, action):
        pl.when(test)(action)

    for k in others:
        gated(rank(targets[k]) < owners, lambda k=k: reduce_copy(k).start())

    @pl.when(me < owners)
    def _():
        r.heap[0] = r.pack[me]
        for k in others:
            reduce_copy(k).wait_recv()
        r.total[...] = jnp.sum(r.heap[...], axis=0)
        for k in others:
            spread_copy(k).start()
        r.summed[me] = r.total[...]

    for k in others:
        gated(rank(sources[k]) < owners, lambda k=k: spread_copy(k).wait_recv())
    place_out(r.summed.at[pl.ds(0, owners)], r.summed_out)
    for copy in started:
        copy.wait_send()
    for k in others:
        gated(rank(targets[k]) < owners, lambda k=k: reduce_copy(k).wait_send())

    @pl.when(me < owners)
    def _():
        for k in others:
            spread_copy(k).wait_send()

    for copy in placed:
        copy.wait()


def exchange(sizes, tokens, cotangent, gain_rows, keys, w1, w2):
    dp, experts, tensor = sizes
    images, count, features = tokens.shape
    units = w1.shape[1]
    slots = experts * SLOT_PER
    pair = 2 if images % 2 == 0 else 1
    chunks = images // pair
    quarter = pair * SLOT_PER
    height = 2 * quarter
    own = experts * quarter
    group = tensor * own
    spread = dp if dp <= 2 else 1
    total = spread * chunks * group
    finish = spread == dp and features % (128 * dp) == 0
    width = features // dp if finish else features
    devices = dp * experts * tensor
    lanes = features // 128
    count_tiles = slots // 8 * lanes + -(-lanes // 8)
    each = -(-count_tiles // devices)
    owners = -(-count_tiles // each)
    perms = tables(pair, experts, tensor)
    dma = pltpu.SemaphoreType.DMA
    vmem = pltpu.VMEM
    ins = dict(x_in=tokens, c_in=cotangent, gain_in=gain_rows, keys_in=keys, w1_in=w1, w2_in=w2,
               mixes_in=perms[0], unp_in=perms[1], ret_in=perms[2], sel_in=perms[3])
    outs = dict(
        stat_out=((images, count, 128), WIDE),
        s_out=((total, width), LOW), g_out=((total, width), LOW),
        h_out=((total, units), LOW), p_out=((total, units), LOW),
        left_out=((images, 4 * slots, count), LOW), right_out=((images, slots, features), LOW),
        moment_out=((images, 8, count), WIDE),
        summed_out=((owners, each * 8, 128), WIDE),
    )
    scratch = dict(
        x=vmem(tokens.shape, LOW), c=vmem(tokens.shape, LOW), normed=vmem(tokens.shape, LOW),
        gain_rows=vmem(gain_rows.shape, WIDE), gains=vmem((1, features), WIDE),
        keys=vmem(keys.shape, LOW), w1=vmem(w1.shape, LOW), w2=vmem(w2.shape, LOW),
        mixes=vmem(perms[0].shape, LOW), unp=vmem(perms[1].shape, LOW),
        turn=vmem(perms[2].shape, LOW), sel=vmem(perms[3].shape, LOW),
        stat=vmem((images, count, 128), WIDE),
        logits=vmem((images, slots, count), WIDE), disp=vmem((images, slots, count), WIDE),
        comb=vmem((images, slots, count), WIDE), slot_in=vmem((images, slots, features), WIDE),
        stack=vmem((2 * pair * slots, features), LOW), found=vmem((2 * pair * slots, features), LOW),
        blk=vmem((chunks, experts, height, features), LOW),
        rows=vmem((chunks, spread, tensor, experts, height, features), LOW),
        s_all=vmem((total, features), LOW), g_all=vmem((total, features), LOW),
        h_all=vmem((total, units), LOW), p_all=vmem((total, units), LOW),
        pre=vmem((chunks * group if spread > 1 else group, units), WIDE),
        part=vmem((chunks, 2, group, features), WIDE),
        sent=vmem((chunks, 2, max(tensor - 1, 1), own, features), LOW),
        got=vmem((chunks, 2, max(tensor - 1, 1), own, features), LOW),
        ret=vmem((chunks, experts, height, features), LOW),
        back=vmem((chunks, experts, height, features), LOW),
        left=vmem((images, 4 * slots, count), LOW), right=vmem((images, slots, features), LOW),
        moment=vmem((images, 8, count), WIDE),
        keys_sum=vmem((slots, features), WIDE), gain_sum=vmem((slots, features), WIDE),
        pack=vmem((owners if owners > devices else devices, each * 8, 128), WIDE),
        heap=vmem((devices, each * 8, 128), WIDE), total=vmem((each * 8, 128), WIDE),
        summed=vmem((devices, each * 8, 128), WIDE),
        in_sem=dma((8,)), image_sem=dma((2, images)), out_sem=dma((len(outs),)),
        zs=dma((chunks, experts)), zr=dma((chunks, experts)),
        ys=dma((chunks, tensor, experts)), yr=dma((chunks, tensor, experts)),
        xs=dma((chunks, tensor, spread)), xr=dma((chunks, tensor, spread)),
        ps=dma((chunks, 2, tensor)), pr=dma((chunks, 2, tensor)),
        bs=dma((chunks, experts)), br=dma((chunks, experts)),
        ss=dma((devices,)), sr=dma((devices,)), gs=dma((devices,)), gr=dma((devices,)),
    )
    far = pl.BlockSpec(memory_space=pltpu.HBM)
    names = list(ins) + list(outs) + list(scratch)
    values = pl.pallas_call(
        functools.partial(exchange_kernel, sizes, spread, names),
        out_shape=[jax.ShapeDtypeStruct(shape, kind) for shape, kind in outs.values()],
        in_specs=[far] * len(ins),
        out_specs=[far] * len(outs),
        scratch_shapes=list(scratch.values()),
        compiler_params=pltpu.CompilerParams(
            collective_id=0, has_side_effects=True, vmem_limit_bytes=56 * 1024 * 1024
        ),
        name="exchange",
    )(*ins.values())
    return dict(zip(outs, values)), finish


def finish_kernel(sizes, names, *refs):
    r = types.SimpleNamespace(**dict(zip(names, refs)))
    images, count, features = r.x.shape
    slots = r.keys.shape[0]
    lanes = features // 128
    products = hasattr(r, "s_in")
    fetched = {}

    def fetch(key, src, dst):
        fetched[key] = pltpu.make_async_copy(src, dst, r.in_sem.at[len(fetched)])
        fetched[key].start()

    if products:
        for key in ("s", "p", "h", "g"):
            fetch(key, getattr(r, key + "_in"), getattr(r, key))
    fetch("keys", r.keys_in, r.keys)
    fetch("gain", r.gain_in, r.gain_rows)
    fetch("moment", r.moment_in, r.moment)
    fetch("left", r.left_in, r.left)
    fetch("right", r.right_in, r.right)
    fetch("stat", r.stat_in, r.stat)
    fetch("summed", r.summed_in, r.summed)

    def image_copy(b, n):
        return pltpu.make_async_copy(
            (r.x_in, r.c_in)[n].at[b], (r.x, r.c)[n].at[b], r.image_sem.at[n, b])

    for b in range(images):
        image_copy(b, 0).start()
        image_copy(b, 1).start()

    placed = []

    def place_out(src, dst):
        copy = pltpu.make_async_copy(src, dst, r.out_sem.at[len(placed)])
        copy.start()
        placed.append(copy)

    if products:
        units = r.p.shape[1]
        fetched["s"].wait()
        r.turned[...] = r.s[...].T
        fetched["p"].wait()

        @pl.loop(0, units // TILE)
        def _(n):
            cols = pl.ds(pl.multiple_of(n * TILE, TILE), TILE)
            r.gin[:, cols] = jnp.dot(
                r.turned[...], r.p[:, cols], preferred_element_type=WIDE).astype(LOW)

        place_out(r.gin, r.gin_out)
        fetched["h"].wait()
        fetched["g"].wait()

        @pl.loop(0, units // TILE)
        def _(n):
            cols = pl.ds(pl.multiple_of(n * TILE, TILE), TILE)
            r.gout[cols, :] = contract_rows(r.h[:, cols], r.g[...]).astype(LOW)

        place_out(r.gout, r.gout_out)
    for key in ("keys", "gain", "moment", "left", "right", "stat", "summed"):
        fetched[key].wait()
    each = r.summed.shape[1] // 8
    bands = slots // 8
    for n in range(bands * lanes):
        band, lane = n // lanes, n % lanes
        r.keys_sum[band * 8:band * 8 + 8, lane * 128:lane * 128 + 128] = r.summed[
            n // each, pl.ds(n % each * 8, 8), :]
    for n in range(lanes):
        m = bands * lanes + n // 8
        row = m % each * 8 + n % 8
        r.gain_sum[n:n + 1, :] = r.summed[m // each, row:row + 1, :]
    place_out(r.keys_sum, r.keys_out)
    place_out(r.gain_sum, r.gain_out)
    r.gains[...] = jnp.concatenate([r.gain_rows[n:n + 1, :] for n in range(lanes)], axis=1)

    @pl.loop(0, images)
    def _(b):
        moment = r.moment[b].T
        average, inverse = r.stat[b, :, 0:1], r.stat[b, :, 1:2]
        r.cols[0] = jnp.broadcast_to(average, (count, 128))
        r.cols[1] = jnp.broadcast_to(inverse, (count, 128))
        r.cols[2] = jnp.broadcast_to(moment[:, 0:1], (count, 128))
        r.cols[3] = jnp.broadcast_to(-inverse * inverse * moment[:, 1:2], (count, 128))
        image_copy(b, 0).wait()
        image_copy(b, 1).wait()
        key = r.keys[...]
        r.weights[0:slots, :] = r.right[b]
        for n in range(1, 4):
            r.weights[n * slots:(n + 1) * slots, :] = key

        @pl.loop(0, lanes)
        def _(n):
            cols = pl.ds(pl.multiple_of(n * 128, 128), 128)
            grads = contract_rows(r.left[b], r.weights[:, cols]) * r.gains[:, cols]
            scaled = (r.x[b, :, cols].astype(WIDE) - r.cols[0]) * r.cols[3]
            change = r.cols[1] * (grads - r.cols[2]) + scaled
            r.out[b, :, cols] = (r.c[b, :, cols].astype(WIDE) + change).astype(LOW)

        pltpu.make_async_copy(r.out.at[b], r.tokens_out.at[b], r.image_out.at[b]).start()

    for copy in placed:
        copy.wait()
    for b in range(images):
        pltpu.make_async_copy(r.out.at[b], r.tokens_out.at[b], r.image_out.at[b]).wait()


def finish_up(sizes, tokens, cotangent, gain_rows, keys, mid, products):
    images, count, features = tokens.shape
    slots = keys.shape[0]
    dma, vmem = pltpu.SemaphoreType.DMA, pltpu.VMEM
    ins = dict(x_in=tokens, c_in=cotangent, gain_in=gain_rows, keys_in=keys,
               stat_in=mid["stat_out"], left_in=mid["left_out"], right_in=mid["right_out"],
               moment_in=mid["moment_out"], summed_in=mid["summed_out"])
    outs = dict(tokens_out=(tokens.shape, LOW), gain_out=(gain_rows.shape, WIDE),
                keys_out=(keys.shape, WIDE))
    scratch = dict(
        x=vmem(tokens.shape, LOW), c=vmem(tokens.shape, LOW), out=vmem(tokens.shape, LOW),
        gain_rows=vmem(gain_rows.shape, WIDE), gains=vmem((1, features), WIDE),
        keys=vmem(keys.shape, LOW), weights=vmem((4 * slots, features), LOW),
        cols=vmem((4, count, 128), WIDE),
        keys_sum=vmem(keys.shape, WIDE), gain_sum=vmem(gain_rows.shape, WIDE),
        in_sem=dma((16,)), image_sem=dma((2, images)), image_out=dma((images,)), out_sem=dma((4,)),
    )
    for key in ("stat", "left", "right", "moment", "summed"):
        scratch[key] = vmem(mid[key + "_out"].shape, mid[key + "_out"].dtype)
    if products:
        for key in ("s", "g", "h", "p"):
            ins[key + "_in"] = mid[key + "_out"]
            scratch[key] = vmem(mid[key + "_out"].shape, LOW)
        total, width = mid["s_out"].shape
        units = mid["p_out"].shape[1]
        scratch.update(turned=vmem((width, total), LOW), gin=vmem((width, units), LOW),
                       gout=vmem((units, width), LOW))
        outs.update(gin_out=((width, units), LOW), gout_out=((units, width), LOW))
    far = pl.BlockSpec(memory_space=pltpu.HBM)
    names = list(ins) + list(outs) + list(scratch)
    return pl.pallas_call(
        functools.partial(finish_kernel, sizes, names),
        out_shape=[jax.ShapeDtypeStruct(shape, kind) for shape, kind in outs.values()],
        in_specs=[far] * len(ins),
        out_specs=[far] * len(outs),
        scratch_shapes=list(scratch.values()),
        compiler_params=pltpu.CompilerParams(vmem_limit_bytes=56 * 1024 * 1024),
        name="finish",
    )(*ins.values())


def local(sizes, tokens, cotangent, norm_gain, slot_keys, w_in, w_out):
    dp = sizes[0]
    features = tokens.shape[2]
    gain_rows, keys = norm_gain.reshape(features // 128, 128), slot_keys.T
    mid, finish = exchange(sizes, tokens, cotangent, gain_rows, keys, w_in[0], w_out[0])
    grad_tokens, grad_gain, grad_keys, *rest = finish_up(
        sizes, tokens, cotangent, gain_rows, keys, mid, finish)
    if finish:
        first_total, second_total = rest
    else:
        slot_rows, grad_rows, hidden, grad_pre = (mid[k + "_out"] for k in ("s", "g", "h", "p"))
        if dp > 2:
            slot_rows = lax.all_to_all(slot_rows, "dp", split_axis=1, concat_axis=0, tiled=True)
            grad_rows = lax.all_to_all(grad_rows, "dp", split_axis=1, concat_axis=0, tiled=True)
            hidden = lax.all_gather(hidden, "dp", axis=0, tiled=True)
            grad_pre = lax.all_gather(grad_pre, "dp", axis=0, tiled=True)
        else:
            width = features // dp
            start = lax.axis_index("dp") * width
            slot_rows = lax.dynamic_slice_in_dim(slot_rows, start, width, axis=1)
            grad_rows = lax.dynamic_slice_in_dim(grad_rows, start, width, axis=1)
        first_total = contract_rows(slot_rows, grad_pre).astype(LOW)
        second_total = contract_rows(hidden, grad_rows).astype(LOW)
    return (
        grad_tokens, grad_gain.reshape(features), grad_keys.T,
        first_total[None], second_total[None],
    )


def solution(mesh):
    tokens = P(("dp", "expert", "tensor"), None, None)
    return jax.shard_map(
        functools.partial(local, tuple(mesh.shape[name] for name in AXES)),
        mesh=mesh,
        in_specs=(tokens, tokens, P(), P(), P("expert", None, "tensor"), P("expert", "tensor", None)),
        out_specs=(tokens, P(), P(), P("expert", "dp", "tensor"), P("expert", "tensor", "dp")),
        check_vma=False,
    )
```

```python
import functools
import types

import jax
import jax.numpy as jnp
from jax import lax
from jax.experimental import pallas as pl
from jax.experimental.pallas import tpu as pltpu
from jax.sharding import PartitionSpec as P

AXES = ("dp", "expert", "tensor")
MESH = pl.DeviceIdType.MESH
SLOT_PER = 2
EPSILON = 1e-06
GELU_A = 0.7978845608028654
GELU_B = 0.044715
TILE = 256
ROWS = 64
LOW, WIDE = jnp.bfloat16, jnp.float32
LIMIT = 40 * 1024 * 1024


def contract_rows(left, right):
    return lax.dot_general(left, right, (((0,), (0,)), ((), ())), preferred_element_type=WIDE)


def contract_cols(left, right):
    return lax.dot_general(left, right, (((1,), (1,)), ((), ())), preferred_element_type=WIDE)


def gelu_of(x):
    return 0.5 * x * (1.0 + jnp.tanh(GELU_A * (x + GELU_B * (x * x * x))))


def gelu_slope(x):
    square = x * x
    bend = jnp.tanh(GELU_A * (x + GELU_B * (square * x)))
    return 0.5 * (1.0 + bend) + 0.5 * x * (1.0 - bend * bend) * (
        GELU_A * (1.0 + 3.0 * GELU_B * square)
    )


def around(position, step, size):
    return lax.rem(position + (step + size), size)


def orders(pair, experts, tensor):
    slots, quarter = experts * SLOT_PER, pair * SLOT_PER
    height, own = 2 * quarter, experts * quarter
    group = tensor * own

    def hot(size, source):
        row = lax.broadcasted_iota(jnp.int32, (size, size), 0)
        return (source(row) == lax.broadcasted_iota(jnp.int32, (size, size), 1)).astype(LOW)

    def image_order(r):
        e, stream, u = r // height, r % height // quarter, r % quarter
        return stream * (pair * slots) + u // SLOT_PER * slots + e * SLOT_PER + u % SLOT_PER

    def stream_order(r):
        e, stream, u = r // height, r % height // quarter, r % quarter
        return stream * own + e * quarter + u

    def block_order(r):
        return r % group // quarter * height + r // group * quarter + r % quarter

    def back_order(r):
        image, stream, slot = r // (2 * slots), r % (2 * slots) // slots, r % slots
        return slot // SLOT_PER * height + stream * quarter + image * SLOT_PER + slot % SLOT_PER

    rows = experts * height
    sizes = (rows, 2 * group, rows, rows)
    sources = (image_order, block_order, stream_order, back_order)
    return [functools.partial(hot, *pair) for pair in zip(sizes, sources)]


def exchange_kernel(sizes, spread, finish, names, *refs):
    dp, experts, tensor = sizes
    r = types.SimpleNamespace(**dict(zip(names, refs)))
    d, e, t = (lax.axis_index(name) for name in AXES)
    images, count, features = r.x.shape
    slots, units = r.keys.shape[0], r.w1.shape[1]
    chunks, _, height, _ = r.blk.shape
    pair, quarter = images // chunks, height // 2
    own = experts * quarter
    group = tensor * own
    lanes = features // 128
    mine = d if spread > 1 else 0
    where = [d, e, t]

    def push(src, dst, send, recv, axis, place):
        target = {"dp": d, "expert": e, "tensor": t}
        target[axis] = place
        return pltpu.make_async_remote_copy(
            src_ref=src, dst_ref=dst, send_sem=send, recv_sem=recv,
            device_id=tuple(target[name] for name in AXES), device_id_type=MESH,
        )

    def columns(tile, extent=features):
        return [slice(n, n + tile) for n in range(0, extent, tile)]

    started = []

    def launch(copy):
        copy.start()
        started.append(copy)

    offsets = [(a, b, c) for a in range(dp) for b in range(experts) for c in range(tensor)]
    targets = [tuple(around(w, k, s) for w, k, s in zip(where, step, sizes)) for step in offsets]
    sources = [tuple(around(w, -k, s) for w, k, s in zip(where, step, sizes)) for step in offsets]
    others = range(1, len(offsets))
    rank = lambda p: (p[0] * experts + p[1]) * tensor + p[2]

    fetched = []

    def fetch(src, dst):
        copy = pltpu.make_async_copy(src, dst, r.in_sem.at[len(fetched)])
        copy.start()
        fetched.append(copy)
        return copy

    def image_copy(b, n):
        return pltpu.make_async_copy(
            (r.x_in, r.c_in)[n].at[b], (r.x, r.c)[n].at[b], r.image_sem.at[n, b])

    small = [fetch(r.gain_in, r.gain_rows), fetch(r.keys_in, r.keys)]
    for b in range(pair):
        image_copy(b, 0).start()
        image_copy(b, 1).start()
    barrier = pltpu.get_barrier_semaphore()
    for k in others:
        pl.semaphore_signal(barrier, inc=1, device_id=targets[k], device_id_type=MESH)
    for b in range(pair, images):
        image_copy(b, 0).start()
        image_copy(b, 1).start()
    w1_copy, w2_copy = fetch(r.w1_in, r.w1), fetch(r.w2_in, r.w2)
    image_order, block_order, stream_order, back_order = orders(pair, experts, tensor)
    for copy in small:
        copy.wait()
    r.gains[...] = jnp.concatenate([r.gain_rows[n:n + 1, :] for n in range(lanes)], axis=1)
    r.keys_sum[...] = jnp.zeros_like(r.keys_sum)
    r.gain_sum[...] = jnp.zeros_like(r.gain_sum)

    def normalise(b):
        blocks = [slice(n, n + ROWS) for n in range(0, count, ROWS)]
        for rows in blocks:
            average = jnp.mean(r.x[b, rows, :].astype(WIDE), axis=-1, keepdims=True)
            r.average[b, rows, :] = jnp.broadcast_to(average, (ROWS, 128))
        for rows in blocks:
            average = r.average[b, rows, :]
            square = jnp.zeros((ROWS, 128), WIDE)
            for lane in columns(128):
                centred = r.x[b, rows, lane].astype(WIDE) - average
                square = square + centred * centred
            spread_of = jnp.sum(square, axis=-1, keepdims=True) * (1.0 / features)
            r.inverse[b, rows, :] = jnp.broadcast_to(lax.rsqrt(spread_of + EPSILON), (ROWS, 128))
        for rows in blocks:
            average, inverse = r.average[b, rows, :], r.inverse[b, rows, :]
            for lane in columns(128):
                centred = r.x[b, rows, lane].astype(WIDE) - average
                r.normed[b, rows, lane] = (centred * inverse * r.gains[:, lane]).astype(LOW)

    def mix_image(b, slab):
        logits = contract_cols(r.keys[...], r.normed[b])
        over_tokens = jnp.exp(logits - jnp.max(logits, axis=1, keepdims=True))
        over_tokens = over_tokens / jnp.sum(over_tokens, axis=1, keepdims=True)
        over_slots = jnp.exp(logits - jnp.max(logits, axis=0, keepdims=True))
        over_slots = over_slots / jnp.sum(over_slots, axis=0, keepdims=True)
        r.logits[b] = logits
        r.disp[b] = over_tokens
        r.comb[b] = over_slots
        taken = jnp.dot(over_tokens.astype(LOW), r.normed[b], preferred_element_type=WIDE)
        given = jnp.dot(over_slots.astype(LOW), r.c[b], preferred_element_type=WIDE)
        r.slot_in[b] = taken
        r.stack[slab * slots:(slab + 1) * slots, :] = taken.astype(LOW)
        r.stack[(pair + slab) * slots:(pair + slab + 1) * slots, :] = given.astype(LOW)

    def mix(c):
        if c == 0:
            r.mixes[...] = image_order()
        for slab in range(pair):
            image_copy(c * pair + slab, 0).wait()
            image_copy(c * pair + slab, 1).wait()
        for slab in range(pair):
            normalise(c * pair + slab)
        for slab in range(pair):
            mix_image(c * pair + slab, slab)
        moved = jnp.dot(r.mixes[...], r.stack[...], preferred_element_type=WIDE)
        for n in range(experts):
            r.blk[c, n] = moved[n * height:(n + 1) * height].astype(LOW)

    near = sorted(range(1, experts), key=lambda k: -min(k, experts - k))
    arrive = {}

    def scatter(c):
        for k in near:
            to = around(e, k, experts)
            arrive[c, k] = push(r.blk.at[c, to], r.rows.at[c, mine, t, e],
                                r.zs.at[c, k], r.zr.at[c, k], "expert", to)
            launch(arrive[c, k])
        share_rows(c, r.blk.at[c, e], 0)
        r.rows[c, mine, t, e] = r.blk[c, e]

    def share_rows(c, src, k):
        slot = r.rows.at[c, mine, t, around(e, -k, experts)]
        for j in range(1, tensor):
            launch(push(src, slot, r.ys.at[c, j, k], r.yr.at[c, j, k], "tensor", around(t, j, tensor)))

    def share_slab(c, j):
        for i in range(1, spread):
            slab = r.rows.at[c, mine, around(t, -j, tensor)]
            launch(push(slab, slab, r.xs.at[c, j, i], r.xr.at[c, j, i], "dp", around(d, i, dp)))

    def forward_rows(c):
        for k in near:
            arrive[c, k].wait_recv()
            share_rows(c, r.rows.at[c, mine, t, around(e, -k, experts)], k)
        share_slab(c, 0)

    def gather_rows(c):
        for j in range(1, tensor):
            for k in [0] + near:
                slot = r.rows.at[c, mine, around(t, -j, tensor), around(e, -k, experts)]
                push(slot, slot, r.ys.at[c, j, k], r.yr.at[c, j, k],
                     "tensor", around(t, j, tensor)).wait_recv()
            share_slab(c, j)

    def unpack(c, place, base):
        block = r.rows[c, place].reshape(2 * group, features)
        both = jnp.dot(r.unp[...], block, preferred_element_type=WIDE)
        r.s_all[base:base + group, :] = both[0:group].astype(LOW)
        r.g_all[base:base + group, :] = both[group:].astype(LOW)

    def transpose(weight, turned):
        row = lax.broadcasted_iota(jnp.int32, (TILE, TILE), 0)
        eye = (row == lax.broadcasted_iota(jnp.int32, (TILE, TILE), 1)).astype(LOW)

        @pl.loop(0, weight.shape[0] // TILE)
        def _(n):
            rows = pl.ds(pl.multiple_of(n * TILE, TILE), TILE)
            for cols in columns(TILE, weight.shape[1]):
                turned[cols, rows] = contract_cols(eye, weight[rows, cols]).astype(LOW)

    def forward(base, size):
        for cols in columns(TILE, units):
            x = jnp.dot(r.s_all[base:base + size, :], r.w1[:, cols], preferred_element_type=WIDE)
            r.pre[0:size, cols] = x
            r.h_all[base:base + size, cols] = gelu_of(x).astype(LOW)

    def backward(base, size):
        for cols in columns(TILE, units):
            x = jnp.dot(r.g_all[base:base + size, :], r.w2_turned[:, cols], preferred_element_type=WIDE)
            r.p_all[base:base + size, cols] = (x * gelu_slope(r.pre[0:size, cols])).astype(LOW)

    def project(c, base):
        for cols in columns(TILE):
            r.part[c, 0, :, cols] = jnp.dot(
                r.h_all[base:base + group, :], r.w2[:, cols], preferred_element_type=WIDE)
        share_part(c, 0)

    def project_back(c, base):
        for cols in columns(TILE):
            r.part[c, 1, :, cols] = jnp.dot(
                r.p_all[base:base + group, :], r.w1_turned[:, cols], preferred_element_type=WIDE)
        share_part(c, 1)

    def part_copy(c, which, j):
        return push(r.sent.at[c, which, j - 1], r.got.at[c, which, j - 1],
                    r.ps.at[c, which, j], r.pr.at[c, which, j], "tensor", around(t, j, tensor))

    def share_part(c, which):
        for j in range(1, tensor):
            to = around(t, j, tensor)
            r.sent[c, which, j - 1] = r.part[c, which, pl.ds(pl.multiple_of(to * own, 8), own), :].astype(LOW)
            launch(part_copy(c, which, j))

    def give_back(c):
        totals = []
        for which in range(2):
            total = r.part[c, which, pl.ds(pl.multiple_of(t * own, 8), own), :]
            for j in range(1, tensor):
                part_copy(c, which, j).wait_recv()
                total = total + r.got[c, which, j - 1].astype(WIDE)
            totals.append(total.astype(LOW))
        moved = jnp.dot(r.turn[...], jnp.concatenate(totals, axis=0), preferred_element_type=WIDE)
        for n in range(experts):
            r.ret[c, n] = moved[n * height:(n + 1) * height].astype(LOW)
        for k in near:
            to = around(e, k, experts)
            arrive["back", c, k] = push(r.ret.at[c, to], r.back.at[c, e],
                                        r.bs.at[c, k], r.br.at[c, k], "expert", to)
            launch(arrive["back", c, k])
        r.back[c, e] = r.ret[c, e]

    def image_gradients(b, slab):
        start = slab * 2 * slots
        returned = r.found[start:start + slots, :]
        slot_grad = r.found[start + slots:start + 2 * slots, :]
        grad_dispatch = contract_cols(slot_grad, r.normed[b])
        grad_combine = contract_cols(returned, r.c[b])
        dispatch, combine = r.disp[b], r.comb[b]
        logit = dispatch * (
            grad_dispatch - jnp.sum(dispatch * grad_dispatch, axis=1, keepdims=True)
        ) + combine * (grad_combine - jnp.sum(combine * grad_combine, axis=0, keepdims=True))
        first = logit.astype(LOW)
        rest = logit - first.astype(WIDE)
        second = rest.astype(LOW)
        third = (rest - second.astype(WIDE)).astype(LOW)
        low = dispatch.astype(LOW)
        split = jnp.concatenate([first, second, third], axis=0)
        r.left[b, 0:slots, :] = low
        r.left[b, slots:4 * slots, :] = split
        r.right[b] = slot_grad
        parts = jnp.dot(split, r.normed[b], preferred_element_type=WIDE)
        r.keys_sum[...] += parts[0:slots] + parts[slots:2 * slots] + parts[2 * slots:3 * slots]
        wide = slot_grad.astype(WIDE)
        r.gain_sum[...] += wide * r.slot_in[b]
        low = low.astype(WIDE)
        gains = r.gains[...]
        from_slots = jnp.sum(wide * gains, axis=1, keepdims=True)
        from_keys = jnp.sum(r.keys[...].astype(WIDE) * gains, axis=1, keepdims=True)
        first_mean = jnp.sum(low * from_slots + logit * from_keys, axis=0, keepdims=True)
        second_mean = jnp.sum(low * grad_dispatch + logit * r.logits[b], axis=0, keepdims=True)
        row = lax.broadcasted_iota(jnp.int32, (8, count), 0)
        r.moment[b] = jnp.where(row == 0, first_mean, second_mean) * (1.0 / features)

    def take_back(c):
        with jax.named_scope(f"waitback{c}"):
            for k in near:
                arrive["back", c, k].wait_recv()
        block = r.back[c].reshape(experts * height, features)
        r.found[...] = jnp.dot(r.sel[...], block, preferred_element_type=WIDE).astype(LOW)

        for slab in range(pair):
            image_gradients(c * pair + slab, slab)

    placed = []

    def place_out(src, dst):
        copy = pltpu.make_async_copy(src, dst, r.out_sem.at[len(placed)])
        copy.start()
        placed.append(copy)

    def finish_image(b):
        moment = r.moment[b].T
        average, inverse = r.average[b], r.inverse[b]
        first = jnp.broadcast_to(moment[:, 0:1], (count, 128))
        second = -inverse * inverse * moment[:, 1:2]
        r.cols[0] = first
        r.cols[1] = second
        left = r.left[b].T
        key = r.keys[...]
        for cols in columns(TILE):
            right = jnp.concatenate([r.right[b, :, cols]] + [key[:, cols]] * 3, axis=0)
            grads = jnp.dot(left, right, preferred_element_type=WIDE) * r.gains[:, cols]
            for n in range(0, TILE, 128):
                lane = slice(cols.start + n, cols.start + n + 128)
                scaled = (r.x[b, :, lane].astype(WIDE) - r.average[b]) * r.cols[1]
                change = r.inverse[b] * (grads[:, n:n + 128] - r.cols[0]) + scaled
                r.x[b, :, lane] = (r.c[b, :, lane].astype(WIDE) + change).astype(LOW)

    full = chunks * group

    def other_rows(i):
        other = around(d, -i, dp)
        for c in range(chunks):
            for j in range(tensor):
                slab = r.rows.at[c, other, around(t, -j, tensor)]
                push(slab, slab, r.xs.at[c, j, i], r.xr.at[c, j, i], "dp", around(d, i, dp)).wait_recv()
            unpack(c, other, i * full + c * group)

    scope = jax.named_scope
    steps = []

    def step(name, action):
        with scope(name):
            action()

    def turn_weight(copy, weight, turned):
        copy.wait()
        transpose(weight, turned)

    last = chunks - 1
    for c in range(chunks):
        step(f"mix{c}", lambda: mix(c))
        if c == 0:
            step("barrier", lambda: pl.semaphore_wait(barrier, len(others)))
        step(f"scatter{c}", lambda: scatter(c))
    step("fwdrows0", lambda: forward_rows(0))
    r.unp[...], r.turn[...], r.sel[...] = block_order(), stream_order(), back_order()
    step("weights2", lambda: turn_weight(w2_copy, r.w2, r.w2_turned))
    if chunks > 1:
        step("fwdrows1", lambda: forward_rows(1))
    step("weights1", lambda: turn_weight(w1_copy, r.w1, r.w1_turned))
    for c in range(chunks):
        base = c * group
        step(f"gather{c}", lambda: gather_rows(c))
        step(f"unpack{c}", lambda: unpack(c, mine, base))
        step(f"forward{c}", lambda: forward(base, group))
        step(f"project{c}", lambda: project(c, base))
        if c + 2 < chunks:
            step(f"fwdrows{c + 2}", lambda: forward_rows(c + 2))
        step(f"backward{c}", lambda: backward(base, group))
        step(f"projback{c}", lambda: project_back(c, base))
        if c > 0:
            step(f"giveback{c - 1}", lambda: give_back(c - 1))
    if chunks > 2:
        step("takeback0", lambda: take_back(0))
    for i in range(1, spread):
        step("otherrows", lambda: other_rows(i))
        step("otherfwd", lambda: forward(i * full, full))
    step(f"giveback{last}", lambda: give_back(last))
    for c in range(1 if chunks > 2 else 0, last):
        step(f"takeback{c}", lambda: take_back(c))
    for i in range(1, spread):
        step("otherbwd", lambda: backward(i * full, full))
    if finish:
        width = r.gin.shape[0]
        mine_cols = pl.ds(pl.multiple_of(d * width, 128), width)

        def product_in():
            r.turned[...] = r.s_all[:, mine_cols].T

            @pl.loop(0, units // TILE)
            def _(n):
                cols = pl.ds(pl.multiple_of(n * TILE, TILE), TILE)
                r.gin[:, cols] = jnp.dot(
                    r.turned[...], r.p_all[:, cols], preferred_element_type=WIDE).astype(LOW)

        def product_out():
            @pl.loop(0, units // TILE)
            def _(n):
                cols = pl.ds(pl.multiple_of(n * TILE, TILE), TILE)
                r.gout[cols, :] = contract_rows(r.h_all[:, cols], r.g_all[:, mine_cols]).astype(LOW)

        step("productin", product_in)
    else:
        place_out(r.s_all, r.s_out)
        place_out(r.g_all, r.g_out)
        place_out(r.h_all, r.h_out)
        place_out(r.p_all, r.p_out)
    step(f"takeback{last}", lambda: take_back(last))

    each = r.pack.shape[1] // 8
    bands = slots // 8
    count_tiles = bands * lanes + -(-lanes // 8)
    owners = -(-count_tiles // each)
    me = rank(where)
    gain = jnp.sum(r.gain_sum[...] + r.keys[...].astype(WIDE) * r.keys_sum[...], axis=0, keepdims=True)
    gain = gain / r.gains[...]
    for n in range(bands * lanes):
        band, lane = n // lanes, n % lanes
        r.pack[n // each, pl.ds(n % each * 8, 8), :] = r.keys_sum[
            band * 8:band * 8 + 8, lane * 128:lane * 128 + 128]
    for n in range(-(-lanes // 8) * 8):
        m = bands * lanes + n // 8
        row = m % each * 8 + n % 8
        piece = gain[:, n * 128:n * 128 + 128] if n < lanes else jnp.zeros((1, 128), WIDE)
        r.pack[m // each, row:row + 1, :] = piece

    def reduce_copy(k):
        return pltpu.make_async_remote_copy(
            src_ref=r.pack.at[rank(targets[k])], dst_ref=r.heap.at[k], send_sem=r.ss.at[k],
            recv_sem=r.sr.at[k], device_id=targets[k], device_id_type=MESH)

    def spread_copy(k):
        return pltpu.make_async_remote_copy(
            src_ref=r.total, dst_ref=r.summed.at[me], send_sem=r.gs.at[k],
            recv_sem=r.gr.at[k], device_id=targets[k], device_id_type=MESH)

    def gated(test, action):
        pl.when(test)(action)

    for k in others:
        gated(rank(targets[k]) < owners, lambda k=k: reduce_copy(k).start())

    def finish_images():
        @pl.loop(0, images)
        def _(b):
            finish_image(b)

    step("elem", finish_images)

    def reduce_own():
        @pl.when(me < owners)
        def _():
            r.heap[0] = r.pack[me]
            for k in others:
                reduce_copy(k).wait_recv()
            r.total[...] = jnp.sum(r.heap[...], axis=0)
            for k in others:
                spread_copy(k).start()
            r.summed[me] = r.total[...]

    step("reduceown", reduce_own)
    if finish:
        step("productout", product_out)

    def drain():
        for copy in started:
            copy.wait_send()
        for k in others:
            gated(rank(targets[k]) < owners, lambda k=k: reduce_copy(k).wait_send())

    step("drain", drain)

    def collect():
        for k in others:
            gated(rank(sources[k]) < owners, lambda k=k: spread_copy(k).wait_recv())
        for n in range(bands * lanes):
            band, lane = n // lanes, n % lanes
            r.keys_out[band * 8:band * 8 + 8, lane * 128:lane * 128 + 128] = r.summed[
                n // each, n % each * 8:n % each * 8 + 8, :]
        for n in range(lanes):
            m = bands * lanes + n // 8
            row = m % each * 8 + n % 8
            r.gain_out[n:n + 1, :] = r.summed[m // each, row:row + 1, :]

        @pl.when(me < owners)
        def _():
            for k in others:
                spread_copy(k).wait_send()

        for copy in placed:
            copy.wait()

    step("collect", collect)


def exchange(sizes, tokens, cotangent, gain_rows, keys, w1, w2):
    dp, experts, tensor = sizes
    images, count, features = tokens.shape
    units = w1.shape[1]
    slots = experts * SLOT_PER
    pair = 2 if images % 2 == 0 else 1
    chunks = images // pair
    quarter = pair * SLOT_PER
    height = 2 * quarter
    own = experts * quarter
    group = tensor * own
    spread = dp if dp <= 2 else 1
    total = spread * chunks * group
    finish = spread == dp and features % (128 * dp) == 0
    devices = dp * experts * tensor
    lanes = features // 128
    count_tiles = slots // 8 * lanes + -(-lanes // 8)
    each = -(-count_tiles // devices)
    dma = pltpu.SemaphoreType.DMA
    vmem = pltpu.VMEM
    ins = dict(x_in=tokens, c_in=cotangent, gain_in=gain_rows, keys_in=keys, w1_in=w1, w2_in=w2)
    outs = dict(x=(tokens.shape, LOW), gain_out=(gain_rows.shape, WIDE), keys_out=(keys.shape, WIDE))
    if finish:
        outs.update(gin=((features // dp, units), LOW), gout=((units, features // dp), LOW))
    held = len(outs)
    if not finish:
        outs.update(s_out=((total, features), LOW), g_out=((total, features), LOW),
                    h_out=((total, units), LOW), p_out=((total, units), LOW))
    rows = experts * height
    scratch = dict(
        c=vmem(tokens.shape, LOW), normed=vmem(tokens.shape, LOW),
        gain_rows=vmem(gain_rows.shape, WIDE), gains=vmem((1, features), WIDE),
        keys=vmem(keys.shape, LOW), w1=vmem(w1.shape, LOW), w2=vmem(w2.shape, LOW),
        mixes=vmem((rows, rows), LOW), unp=vmem((2 * group, 2 * group), LOW),
        turn=vmem((rows, rows), LOW), sel=vmem((rows, rows), LOW),
        average=vmem((images, count, 128), WIDE), inverse=vmem((images, count, 128), WIDE),
        cols=vmem((2, count, 128), WIDE),
        w1_turned=vmem(w1.shape[::-1], LOW), w2_turned=vmem(w2.shape[::-1], LOW),
        logits=vmem((images, slots, count), WIDE), disp=vmem((images, slots, count), WIDE),
        comb=vmem((images, slots, count), WIDE), slot_in=vmem((images, slots, features), WIDE),
        stack=vmem((2 * pair * slots, features), LOW), found=vmem((2 * pair * slots, features), LOW),
        blk=vmem((chunks, experts, height, features), LOW),
        rows=vmem((chunks, spread, tensor, experts, height, features), LOW),
        s_all=vmem((total, features), LOW), g_all=vmem((total, features), LOW),
        h_all=vmem((total, units), LOW), p_all=vmem((total, units), LOW),
        pre=vmem((chunks * group if spread > 1 else group, units), WIDE),
        part=vmem((chunks, 2, group, features), WIDE),
        sent=vmem((chunks, 2, max(tensor - 1, 1), own, features), LOW),
        got=vmem((chunks, 2, max(tensor - 1, 1), own, features), LOW),
        ret=vmem((chunks, experts, height, features), LOW),
        back=vmem((chunks, experts, height, features), LOW),
        left=vmem((images, 4 * slots, count), LOW), right=vmem((images, slots, features), LOW),
        moment=vmem((images, 8, count), WIDE),
        keys_sum=vmem((slots, features), WIDE), gain_sum=vmem((slots, features), WIDE),
        pack=vmem((devices, each * 8, 128), WIDE),
        heap=vmem((devices, each * 8, 128), WIDE), total=vmem((each * 8, 128), WIDE),
        summed=vmem((devices, each * 8, 128), WIDE),
        in_sem=dma((8,)), image_sem=dma((2, images)), out_sem=dma((4,)),
        zs=dma((chunks, experts)), zr=dma((chunks, experts)),
        ys=dma((chunks, tensor, experts)), yr=dma((chunks, tensor, experts)),
        xs=dma((chunks, tensor, spread)), xr=dma((chunks, tensor, spread)),
        ps=dma((chunks, 2, tensor)), pr=dma((chunks, 2, tensor)),
        bs=dma((chunks, experts)), br=dma((chunks, experts)),
        ss=dma((devices,)), sr=dma((devices,)), gs=dma((devices,)), gr=dma((devices,)),
    )
    if finish:
        scratch.update(turned=vmem((features // dp, total), LOW))
    far, near = pl.BlockSpec(memory_space=pltpu.HBM), pl.BlockSpec(memory_space=vmem)
    names = list(ins) + list(outs) + list(scratch)
    values = pl.pallas_call(
        functools.partial(exchange_kernel, sizes, spread, finish, names),
        out_shape=[jax.ShapeDtypeStruct(shape, kind) for shape, kind in outs.values()],
        in_specs=[far] * len(ins),
        out_specs=[near] * held + [far] * (len(outs) - held),
        scratch_shapes=list(scratch.values()),
        compiler_params=pltpu.CompilerParams(
            collective_id=0, has_side_effects=True, vmem_limit_bytes=LIMIT if finish else LIMIT + LIMIT // 4
        ),
        name="exchange",
    )(*[pltpu.with_memory_space_constraint(v, pltpu.HBM) for v in ins.values()])
    return values[:held], values[held:]


def store_kernel(count, *refs):
    copies = [
        pltpu.make_async_copy(refs[n], refs[count + n], refs[-1].at[n]) for n in range(count)
    ]
    for copy in copies:
        copy.start()
    for copy in copies:
        copy.wait()


def store(values):
    count = len(values)
    return pl.pallas_call(
        functools.partial(store_kernel, count),
        out_shape=[jax.ShapeDtypeStruct(v.shape, v.dtype) for v in values],
        in_specs=[pl.BlockSpec(memory_space=pltpu.VMEM)] * count,
        out_specs=[pl.BlockSpec(memory_space=pltpu.HBM)] * count,
        scratch_shapes=[pltpu.SemaphoreType.DMA((count,))],
        compiler_params=pltpu.CompilerParams(vmem_limit_bytes=12 * 1024 * 1024),
        name="store",
    )(*values)


def local(sizes, tokens, cotangent, norm_gain, slot_keys, w_in, w_out):
    dp = sizes[0]
    features = tokens.shape[2]
    gain_rows, keys = norm_gain.reshape(features // 128, 128), slot_keys.T
    held, rows = exchange(sizes, tokens, cotangent, gain_rows, keys, w_in[0], w_out[0])
    grad_tokens, grad_gain, grad_keys, *rest = store(held)
    if rest:
        first_total, second_total = rest
    else:
        slot_rows, grad_rows, hidden, grad_pre = rows
        if dp > 2:
            slot_rows = lax.all_to_all(slot_rows, "dp", split_axis=1, concat_axis=0, tiled=True)
            grad_rows = lax.all_to_all(grad_rows, "dp", split_axis=1, concat_axis=0, tiled=True)
            hidden = lax.all_gather(hidden, "dp", axis=0, tiled=True)
            grad_pre = lax.all_gather(grad_pre, "dp", axis=0, tiled=True)
        else:
            width = features // dp
            start = lax.axis_index("dp") * width
            slot_rows = lax.dynamic_slice_in_dim(slot_rows, start, width, axis=1)
            grad_rows = lax.dynamic_slice_in_dim(grad_rows, start, width, axis=1)
        first_total = contract_rows(slot_rows, grad_pre).astype(LOW)
        second_total = contract_rows(hidden, grad_rows).astype(LOW)
    return (
        grad_tokens, grad_gain.reshape(features), grad_keys.T,
        first_total[None], second_total[None],
    )


def solution(mesh):
    tokens = P(("dp", "expert", "tensor"), None, None)
    return jax.shard_map(
        functools.partial(local, tuple(mesh.shape[name] for name in AXES)),
        mesh=mesh,
        in_specs=(tokens, tokens, P(), P(), P("expert", None, "tensor"), P("expert", "tensor", None)),
        out_specs=(tokens, P(), P(), P("expert", "dp", "tensor"), P("expert", "tensor", "dp")),
        check_vma=False,
    )
```

```python
import functools
import types

import jax
import jax.numpy as jnp
from jax import lax
from jax.experimental import pallas as pl
from jax.experimental.pallas import tpu as pltpu
from jax.sharding import PartitionSpec as P

AXES = ("dp", "expert", "tensor")
MESH = pl.DeviceIdType.MESH
SLOT_PER = 2
EPSILON = 1e-06
GELU_A = 0.7978845608028654
GELU_B = 0.044715
TILE = 256
ROWS = 64
LOW, WIDE = jnp.bfloat16, jnp.float32
LIMIT = 40 * 1024 * 1024


def contract_rows(left, right):
    return lax.dot_general(left, right, (((0,), (0,)), ((), ())), preferred_element_type=WIDE)


def contract_cols(left, right):
    return lax.dot_general(left, right, (((1,), (1,)), ((), ())), preferred_element_type=WIDE)


def gelu_of(x):
    return 0.5 * x * (1.0 + jnp.tanh(GELU_A * (x + GELU_B * (x * x * x))))


def gelu_slope(x):
    square = x * x
    bend = jnp.tanh(GELU_A * (x + GELU_B * (square * x)))
    return 0.5 * (1.0 + bend) + 0.5 * x * (1.0 - bend * bend) * (
        GELU_A * (1.0 + 3.0 * GELU_B * square)
    )


def around(position, step, size):
    return lax.rem(position + (step + size), size)


def orders(pair, experts, tensor):
    slots, quarter = experts * SLOT_PER, pair * SLOT_PER
    height, own = 2 * quarter, experts * quarter
    group = tensor * own

    def hot(size, source):
        row = lax.broadcasted_iota(jnp.int32, (size, size), 0)
        return (source(row) == lax.broadcasted_iota(jnp.int32, (size, size), 1)).astype(LOW)

    def image_order(r):
        e, stream, u = r // height, r % height // quarter, r % quarter
        return stream * (pair * slots) + u // SLOT_PER * slots + e * SLOT_PER + u % SLOT_PER

    def stream_order(r):
        e, stream, u = r // height, r % height // quarter, r % quarter
        return stream * own + e * quarter + u

    def block_order(r):
        return r % group // quarter * height + r // group * quarter + r % quarter

    def back_order(r):
        image, stream, slot = r // (2 * slots), r % (2 * slots) // slots, r % slots
        return slot // SLOT_PER * height + stream * quarter + image * SLOT_PER + slot % SLOT_PER

    rows = experts * height
    sizes = (rows, 2 * group, rows, rows)
    sources = (image_order, block_order, stream_order, back_order)
    return [functools.partial(hot, *pair) for pair in zip(sizes, sources)]


def exchange_kernel(sizes, spread, finish, names, *refs):
    dp, experts, tensor = sizes
    r = types.SimpleNamespace(**dict(zip(names, refs)))
    d, e, t = (lax.axis_index(name) for name in AXES)
    images, count, features = r.x.shape
    slots, units = r.keys.shape[0], r.w1.shape[1]
    chunks, _, height, _ = r.blk.shape
    pair, quarter = images // chunks, height // 2
    own = experts * quarter
    group = tensor * own
    lanes = features // 128
    mine = d if spread > 1 else 0
    where = [d, e, t]

    def push(src, dst, send, recv, axis, place):
        target = {"dp": d, "expert": e, "tensor": t}
        target[axis] = place
        return pltpu.make_async_remote_copy(
            src_ref=src, dst_ref=dst, send_sem=send, recv_sem=recv,
            device_id=tuple(target[name] for name in AXES), device_id_type=MESH,
        )

    def columns(tile, extent=features):
        return [slice(n, n + tile) for n in range(0, extent, tile)]

    sent, returned = [], {}

    def launch(copy):
        copy.start()
        sent.append(copy)

    offsets = [(a, b, c) for a in range(dp) for b in range(experts) for c in range(tensor)]
    targets = [tuple(around(w, k, s) for w, k, s in zip(where, step, sizes)) for step in offsets]
    sources = [tuple(around(w, -k, s) for w, k, s in zip(where, step, sizes)) for step in offsets]
    others = range(1, len(offsets))
    rank = lambda p: (p[0] * experts + p[1]) * tensor + p[2]

    fetched = []

    def fetch(src, dst):
        copy = pltpu.make_async_copy(src, dst, r.in_sem.at[len(fetched)])
        copy.start()
        fetched.append(copy)
        return copy

    def image_copy(b, n):
        return pltpu.make_async_copy(
            (r.x_in, r.c_in)[n].at[b], (r.x, r.c)[n].at[b], r.image_sem.at[n, b])

    small = [fetch(r.gain_in, r.gain_rows), fetch(r.keys_in, r.keys)]
    for b in range(pair):
        image_copy(b, 0).start()
        image_copy(b, 1).start()
    barrier = pltpu.get_barrier_semaphore()
    for k in others:
        pl.semaphore_signal(barrier, inc=1, device_id=targets[k], device_id_type=MESH)
    for b in range(pair, images):
        image_copy(b, 0).start()
        image_copy(b, 1).start()
    w1_copy, w2_copy = fetch(r.w1_in, r.w1), fetch(r.w2_in, r.w2)
    image_order, block_order, stream_order, back_order = orders(pair, experts, tensor)
    r.keys_sum[...] = jnp.zeros_like(r.keys_sum)
    r.gain_sum[...] = jnp.zeros_like(r.gain_sum)

    def normalise(b):
        blocks = [slice(n, n + ROWS) for n in range(0, count, ROWS)]
        for rows in blocks:
            average = jnp.mean(r.x[b, rows, :].astype(WIDE), axis=-1, keepdims=True)
            r.average[b, rows, :] = jnp.broadcast_to(average, (ROWS, 128))
        for rows in blocks:
            average = r.average[b, rows, :]
            square = jnp.zeros((ROWS, 128), WIDE)
            for lane in columns(128):
                centred = r.x[b, rows, lane].astype(WIDE) - average
                square = square + centred * centred
            spread_of = jnp.sum(square, axis=-1, keepdims=True) * (1.0 / features)
            r.inverse[b, rows, :] = jnp.broadcast_to(lax.rsqrt(spread_of + EPSILON), (ROWS, 128))
        for rows in blocks:
            average, inverse = r.average[b, rows, :], r.inverse[b, rows, :]
            for lane in columns(128):
                centred = r.x[b, rows, lane].astype(WIDE) - average
                r.normed[b, rows, lane] = (centred * inverse * r.gains[:, lane]).astype(LOW)

    def mix_image(b, slab):
        logits = contract_cols(r.keys[...], r.normed[b])
        over_tokens = jnp.exp(logits - jnp.max(logits, axis=1, keepdims=True))
        over_tokens = over_tokens / jnp.sum(over_tokens, axis=1, keepdims=True)
        over_slots = jnp.exp(logits - jnp.max(logits, axis=0, keepdims=True))
        over_slots = over_slots / jnp.sum(over_slots, axis=0, keepdims=True)
        r.logits[b] = logits
        r.disp[b] = over_tokens
        r.comb[b] = over_slots
        taken = jnp.dot(over_tokens.astype(LOW), r.normed[b], preferred_element_type=WIDE)
        given = jnp.dot(over_slots.astype(LOW), r.c[b], preferred_element_type=WIDE)
        r.slot_in[b] = taken
        r.stack[slab * slots:(slab + 1) * slots, :] = taken.astype(LOW)
        r.stack[(pair + slab) * slots:(pair + slab + 1) * slots, :] = given.astype(LOW)

    def pack_rows(c):
        moved = jnp.dot(r.mixes[...], r.stack[...], preferred_element_type=WIDE)
        for n in range(experts):
            r.blk[c, n] = moved[n * height:(n + 1) * height].astype(LOW)

    def partner(k):
        place = e
        for bit in (1 << n for n in range(k.bit_length()) if k >> n & 1):
            place = place + bit * (1 - 2 * lax.rem(lax.div(e, bit), 2))
        return place

    near = list(range(1, experts))
    if experts & (experts - 1) == 0:
        goes = comes = [partner(k) for k in range(experts)]
    else:
        goes = [around(e, k, experts) for k in range(experts)]
        comes = [around(e, -k, experts) for k in range(experts)]
    arrive = {}

    def scatter(c):
        share_rows(c, r.blk.at[c, e], 0)
        for k in near:
            arrive[c, k] = push(r.blk.at[c, goes[k]], r.rows.at[c, mine, t, e],
                                r.zs.at[c], r.zr.at[c, k], "expert", goes[k])
            arrive[c, k].start()
        most = r.rows.at[c, mine, t, pl.ds(0, experts - 1)]
        sent.append(push(most, most, r.zs.at[c], r.zr.at[c, 1], "expert", goes[1]))
        r.rows[c, mine, t, e] = r.blk[c, e]

    def share_rows(c, src, k):
        slot = r.rows.at[c, mine, t, comes[k]]
        for j in range(1, tensor):
            push(src, slot, r.ys.at[c, j - 1], r.yr.at[c, j - 1], "tensor", around(t, j, tensor)).start()

    def share_slab(c, j):
        for i in range(1, spread):
            slab = r.rows.at[c, mine, around(t, -j, tensor)]
            launch(push(slab, slab, r.xs.at[c, j, i - 1], r.xr.at[c, j, i - 1], "dp", around(d, i, dp)))

    waiting = {}

    def forward_rows(c, upto=experts):
        ready = [k for k in waiting.setdefault(c, list(near)) if k < upto]
        for k in ready:
            waiting[c].remove(k)
            arrive[c, k].wait_recv()
            share_rows(c, r.rows.at[c, mine, t, comes[k]], k)
        if ready and not waiting[c]:
            share_slab(c, 0)

    def gather_rows(c):
        for j in range(1, tensor):
            slab = r.rows.at[c, mine, around(t, -j, tensor)]
            whole = push(slab, slab, r.ys.at[c, j - 1], r.yr.at[c, j - 1], "tensor", around(t, j, tensor))
            whole.wait_recv()
            sent.append(whole)
            share_slab(c, j)

    def unpack(c, place, base):
        block = r.rows[c, place].reshape(2 * group, features)
        both = jnp.dot(r.unp[...], block, preferred_element_type=WIDE)
        r.s_all[base:base + group, :] = both[0:group].astype(LOW)
        r.g_all[base:base + group, :] = both[group:].astype(LOW)

    def transpose(weight, turned):
        row = lax.broadcasted_iota(jnp.int32, (TILE, TILE), 0)
        eye = (row == lax.broadcasted_iota(jnp.int32, (TILE, TILE), 1)).astype(LOW)

        @pl.loop(0, weight.shape[0] // TILE)
        def _(n):
            rows = pl.ds(pl.multiple_of(n * TILE, TILE), TILE)
            for cols in columns(TILE, weight.shape[1]):
                turned[cols, rows] = contract_cols(eye, weight[rows, cols]).astype(LOW)

    def forward(base, size):
        for cols in columns(TILE, units):
            x = jnp.dot(r.s_all[base:base + size, :], r.w1[:, cols], preferred_element_type=WIDE)
            r.pre[0:size, cols] = x
            r.h_all[base:base + size, cols] = gelu_of(x).astype(LOW)

    def backward(base, size):
        for cols in columns(TILE, units):
            x = jnp.dot(r.g_all[base:base + size, :], r.w2_turned[:, cols], preferred_element_type=WIDE)
            r.p_all[base:base + size, cols] = (x * gelu_slope(r.pre[0:size, cols])).astype(LOW)

    def project(c, base):
        for cols in columns(TILE):
            r.part[c, 0, :, cols] = jnp.dot(
                r.h_all[base:base + group, :], r.w2[:, cols], preferred_element_type=WIDE)
        share_part(c, 0)

    def project_back(c, base):
        for cols in columns(TILE):
            r.part[c, 1, :, cols] = jnp.dot(
                r.p_all[base:base + group, :], r.w1_turned[:, cols], preferred_element_type=WIDE)
        share_part(c, 1)

    def part_copy(c, which, j):
        return push(r.sent.at[c, which, j - 1], r.got.at[c, which, j - 1],
                    r.ps.at[c, which, j - 1], r.pr.at[c, which, j - 1], "tensor", around(t, j, tensor))

    def share_part(c, which):
        for j in range(1, tensor):
            to = around(t, j, tensor)
            r.sent[c, which, j - 1] = r.part[c, which, pl.ds(pl.multiple_of(to * own, 8), own), :].astype(LOW)
            launch(part_copy(c, which, j))

    def give_back(c):
        totals = []
        for which in range(2):
            total = r.part[c, which, pl.ds(pl.multiple_of(t * own, 8), own), :]
            for j in range(1, tensor):
                part_copy(c, which, j).wait_recv()
                total = total + r.got[c, which, j - 1].astype(WIDE)
            totals.append(total.astype(LOW))
        moved = jnp.dot(r.turn[...], jnp.concatenate(totals, axis=0), preferred_element_type=WIDE)
        for n in range(experts):
            r.ret[c, n] = moved[n * height:(n + 1) * height].astype(LOW)
        for k in reversed(near):
            push(r.ret.at[c, goes[k]], r.back.at[c, e], r.bs.at[c], r.br.at[c], "expert", goes[k]).start()
        most = r.back.at[c, pl.ds(0, experts - 1)]
        returned[c] = push(most, most, r.bs.at[c], r.br.at[c], "expert", goes[1])
        sent.append(returned[c])
        r.back[c, e] = r.ret[c, e]

    def image_gradients(b, slab):
        start = slab * 2 * slots
        returned = r.found[start:start + slots, :]
        slot_grad = r.found[start + slots:start + 2 * slots, :]
        grad_dispatch = contract_cols(slot_grad, r.normed[b])
        grad_combine = contract_cols(returned, r.c[b])
        dispatch, combine = r.disp[b], r.comb[b]
        logit = dispatch * (
            grad_dispatch - jnp.sum(dispatch * grad_dispatch, axis=1, keepdims=True)
        ) + combine * (grad_combine - jnp.sum(combine * grad_combine, axis=0, keepdims=True))
        first = logit.astype(LOW)
        rest = logit - first.astype(WIDE)
        second = rest.astype(LOW)
        third = (rest - second.astype(WIDE)).astype(LOW)
        low = dispatch.astype(LOW)
        split = jnp.concatenate([first, second, third], axis=0)
        r.left[b, 0:slots, :] = low
        r.left[b, slots:4 * slots, :] = split
        r.right[b] = slot_grad
        parts = jnp.dot(split, r.normed[b], preferred_element_type=WIDE)
        r.keys_sum[...] += parts[0:slots] + parts[slots:2 * slots] + parts[2 * slots:3 * slots]
        wide = slot_grad.astype(WIDE)
        r.gain_sum[...] += wide * r.slot_in[b]
        low = low.astype(WIDE)
        gains = r.gains[...]
        from_slots = jnp.sum(wide * gains, axis=1, keepdims=True)
        from_keys = jnp.sum(r.keys[...].astype(WIDE) * gains, axis=1, keepdims=True)
        first_mean = jnp.sum(low * from_slots + logit * from_keys, axis=0, keepdims=True)
        second_mean = jnp.sum(low * grad_dispatch + logit * r.logits[b], axis=0, keepdims=True)
        row = lax.broadcasted_iota(jnp.int32, (8, count), 0)
        r.moment[b] = jnp.where(row == 0, first_mean, second_mean) * (1.0 / features)

    def take_back(c):
        with jax.named_scope(f"waitback{c}"):
            returned[c].wait_recv()
        block = r.back[c].reshape(experts * height, features)
        r.found[...] = jnp.dot(r.sel[...], block, preferred_element_type=WIDE).astype(LOW)

        for slab in range(pair):
            image_gradients(c * pair + slab, slab)

    placed = []

    def place_out(src, dst):
        copy = pltpu.make_async_copy(src, dst, r.out_sem.at[len(placed)])
        copy.start()
        placed.append(copy)

    def finish_image(b):
        moment = r.moment[b].T
        average, inverse = r.average[b], r.inverse[b]
        first = jnp.broadcast_to(moment[:, 0:1], (count, 128))
        second = -inverse * inverse * moment[:, 1:2]
        r.cols[0] = first
        r.cols[1] = second
        left = r.left[b].T
        key = r.keys[...]
        for cols in columns(TILE):
            right = jnp.concatenate([r.right[b, :, cols]] + [key[:, cols]] * 3, axis=0)
            grads = jnp.dot(left, right, preferred_element_type=WIDE) * r.gains[:, cols]
            for n in range(0, TILE, 128):
                lane = slice(cols.start + n, cols.start + n + 128)
                scaled = (r.x[b, :, lane].astype(WIDE) - r.average[b]) * r.cols[1]
                change = r.inverse[b] * (grads[:, n:n + 128] - r.cols[0]) + scaled
                r.x[b, :, lane] = (r.c[b, :, lane].astype(WIDE) + change).astype(LOW)

    full = chunks * group

    def other_rows(i):
        other = around(d, -i, dp)
        for c in range(chunks):
            for j in range(tensor):
                slab = r.rows.at[c, other, around(t, -j, tensor)]
                push(slab, slab, r.xs.at[c, j, i - 1], r.xr.at[c, j, i - 1], "dp", around(d, i, dp)).wait_recv()
            unpack(c, other, i * full + c * group)

    scope = jax.named_scope

    def step(name, action):
        with scope(name):
            action()

    def weights_ready():
        w1_copy.wait()
        w2_copy.wait()

    def wait_image(b):
        image_copy(b, 0).wait()
        image_copy(b, 1).wait()

    def set_gains():
        for copy in small:
            copy.wait()
        r.gains[...] = jnp.concatenate([r.gain_rows[n:n + 1, :] for n in range(lanes)], axis=1)

    def mix_pair(b, after):
        if after:
            wait_image(b + 1)
            normalise(b + 1)
        mix_image(b, b % pair)
        if b % pair == pair - 1:
            pack_rows(b // pair)

    def start_mix():
        r.mixes[...] = image_order()
        image_copy(0, 0).wait()
        set_gains()
        normalise(0)

    def mix_first():
        image_copy(0, 1).wait()
        for b in range(1, pair):
            wait_image(b)
        for b in range(1, pair):
            normalise(b)
        for b in range(pair):
            mix_image(b, b)
        pack_rows(0)

    last = chunks - 1
    step("start", start_mix)
    quarters = [experts // 4, experts // 2, 3 * experts // 4, experts]
    step("mix01", mix_first)
    for b in range(pair - 1, images):
        c = b // pair
        if b >= pair:
            step(f"mix{b}", lambda: mix_pair(b, b + 1 < images))
        if b % pair == pair - 1:
            if c == 0:
                step("barrier", lambda: pl.semaphore_wait(barrier, len(others)))
            step(f"scatter{c}", lambda: scatter(c))
            if b == pair - 1 and images > pair:
                def more():
                    wait_image(b + 1)
                    normalise(b + 1)
                step("more", more)
        hook = b - pair
        if 0 <= hook < len(quarters) and images > pair:
            step(f"fwd0_{hook}", lambda: forward_rows(0, quarters[hook]))
    step("fwdrows0", lambda: forward_rows(0))
    if chunks > 1:
        step("fwd1_near", lambda: forward_rows(1, experts // 2))
    r.unp[...], r.turn[...], r.sel[...] = block_order(), stream_order(), back_order()
    step("weights", weights_ready)
    step("weights2", lambda: transpose(r.w2, r.w2_turned))
    if chunks > 1:
        step("fwdrows1", lambda: forward_rows(1))
    if chunks > 2:
        step("fwd2_near", lambda: forward_rows(2, experts // 2))
    for c in range(chunks):
        base = c * group
        step(f"gather{c}", lambda: gather_rows(c))
        step(f"unpack{c}", lambda: unpack(c, mine, base))
        step(f"forward{c}", lambda: forward(base, group))
        step(f"project{c}", lambda: project(c, base))
        if c == 0:
            step("weights1", lambda: transpose(r.w1, r.w1_turned))
        if c > 1:
            step(f"giveback{c - 2}", lambda: give_back(c - 2))
        if c + 2 < chunks:
            step(f"fwdrows{c + 2}", lambda: forward_rows(c + 2))
        step(f"backward{c}", lambda: backward(base, group))
        step(f"projback{c}", lambda: project_back(c, base))
    def other_forward():
        for i in range(1, spread):
            step("otherrows", lambda: other_rows(i))
            step("otherfwd", lambda: forward(i * full, full))

    for c in range(max(chunks - 2, 0), chunks):
        step(f"giveback{c}", lambda: give_back(c))
    for c in range(last):
        step(f"takeback{c}", lambda: take_back(c))
        if c == 0:
            other_forward()
    if last == 0:
        other_forward()
    if finish:
        width = r.gin.shape[0]
        mine_cols = pl.ds(pl.multiple_of(d * width, 128), width)

        def product_in():
            r.turned[...] = r.s_all[:, mine_cols].T

            @pl.loop(0, units // TILE)
            def _(n):
                cols = pl.ds(pl.multiple_of(n * TILE, TILE), TILE)
                r.gin[:, cols] = jnp.dot(
                    r.turned[...], r.p_all[:, cols], preferred_element_type=WIDE).astype(LOW)

        def product_out():
            @pl.loop(0, units // TILE)
            def _(n):
                cols = pl.ds(pl.multiple_of(n * TILE, TILE), TILE)
                r.gout[cols, :] = contract_rows(r.h_all[:, cols], r.g_all[:, mine_cols]).astype(LOW)

    step(f"takeback{last}", lambda: take_back(last))

    each = r.pack.shape[1] // 8
    bands = slots // 8
    count_tiles = bands * lanes + -(-lanes // 8)
    owners = -(-count_tiles // each)
    me = rank(where)
    gain = jnp.sum(r.gain_sum[...] + r.keys[...].astype(WIDE) * r.keys_sum[...], axis=0, keepdims=True)
    gain = gain / r.gains[...]
    for n in range(bands * lanes):
        band, lane = n // lanes, n % lanes
        r.pack[n // each, pl.ds(n % each * 8, 8), :] = r.keys_sum[
            band * 8:band * 8 + 8, lane * 128:lane * 128 + 128]
    for n in range(-(-lanes // 8) * 8):
        m = bands * lanes + n // 8
        row = m % each * 8 + n % 8
        piece = gain[:, n * 128:n * 128 + 128] if n < lanes else jnp.zeros((1, 128), WIDE)
        r.pack[m // each, row:row + 1, :] = piece

    def reduce_copy(k):
        return pltpu.make_async_remote_copy(
            src_ref=r.pack.at[rank(targets[k])], dst_ref=r.heap.at[k], send_sem=r.ends.at[0],
            recv_sem=r.ends.at[1], device_id=targets[k], device_id_type=MESH)

    def spread_copy(k):
        return pltpu.make_async_remote_copy(
            src_ref=r.total, dst_ref=r.summed.at[me], send_sem=r.ends.at[2],
            recv_sem=r.ends.at[3], device_id=targets[k], device_id_type=MESH)

    def many(size, n):
        some = r.heap.at[pl.ds(0, size)]
        return pltpu.make_async_remote_copy(
            src_ref=some, dst_ref=some, send_sem=r.ends.at[n], recv_sem=r.ends.at[n + 1],
            device_id=targets[1], device_id_type=MESH)

    def gated(test, action):
        pl.when(test)(action)

    def by_owner(action):
        gated(me < owners, lambda: action(owners - 1))
        gated(me >= owners, lambda: action(owners))

    for k in others:
        gated(rank(targets[k]) < owners, lambda k=k: reduce_copy(k).start())

    def finish_images():
        @pl.loop(0, images)
        def _(b):
            finish_image(b)

    step("elem", finish_images)
    for i in range(1, spread):
        step("otherbwd", lambda: backward(i * full, full))

    def reduce_own():
        @pl.when(me < owners)
        def _():
            r.heap[0] = r.pack[me]
            many(len(others), 0).wait_recv()
            r.total[...] = jnp.sum(r.heap[...], axis=0)
            for k in others:
                spread_copy(k).start()
            r.summed[me] = r.total[...]

    step("reduceown", reduce_own)
    if finish:
        step("productin", product_in)
        step("productout", product_out)
    else:
        place_out(r.s_all, r.s_out)
        place_out(r.g_all, r.g_out)
        place_out(r.h_all, r.h_out)
        place_out(r.p_all, r.p_out)

    def drain():
        for copy in sent:
            copy.wait_send()
        by_owner(lambda size: many(size, 0).wait_send())

    step("drain", drain)

    def collect():
        by_owner(lambda size: many(size, 2).wait_recv())
        for n in range(bands * lanes):
            band, lane = n // lanes, n % lanes
            r.keys_out[band * 8:band * 8 + 8, lane * 128:lane * 128 + 128] = r.summed[
                n // each, n % each * 8:n % each * 8 + 8, :]
        for n in range(lanes):
            m = bands * lanes + n // 8
            row = m % each * 8 + n % 8
            r.gain_out[n:n + 1, :] = r.summed[m // each, row:row + 1, :]

        gated(me < owners, lambda: many(len(others), 2).wait_send())
        for copy in placed:
            copy.wait()

    step("collect", collect)


def exchange(sizes, tokens, cotangent, gain_rows, keys, w1, w2):
    dp, experts, tensor = sizes
    images, count, features = tokens.shape
    units = w1.shape[1]
    slots = experts * SLOT_PER
    pair = 2 if images % 2 == 0 else 1
    chunks = images // pair
    quarter = pair * SLOT_PER
    height = 2 * quarter
    own = experts * quarter
    group = tensor * own
    spread = dp if dp <= 2 else 1
    total = spread * chunks * group
    finish = spread == dp and features % (128 * dp) == 0
    devices = dp * experts * tensor
    lanes = features // 128
    count_tiles = slots // 8 * lanes + -(-lanes // 8)
    each = -(-count_tiles // devices)
    dma = pltpu.SemaphoreType.DMA
    vmem = pltpu.VMEM
    ins = dict(x_in=tokens, c_in=cotangent, gain_in=gain_rows, keys_in=keys, w1_in=w1, w2_in=w2)
    outs = dict(x=(tokens.shape, LOW), gain_out=(gain_rows.shape, WIDE), keys_out=(keys.shape, WIDE))
    if finish:
        outs.update(gin=((features // dp, units), LOW), gout=((units, features // dp), LOW))
    held = len(outs)
    if not finish:
        outs.update(s_out=((total, features), LOW), g_out=((total, features), LOW),
                    h_out=((total, units), LOW), p_out=((total, units), LOW))
    rows = experts * height
    scratch = dict(
        c=vmem(tokens.shape, LOW), normed=vmem(tokens.shape, LOW),
        gain_rows=vmem(gain_rows.shape, WIDE), gains=vmem((1, features), WIDE),
        keys=vmem(keys.shape, LOW), w1=vmem(w1.shape, LOW), w2=vmem(w2.shape, LOW),
        mixes=vmem((rows, rows), LOW), unp=vmem((2 * group, 2 * group), LOW),
        turn=vmem((rows, rows), LOW), sel=vmem((rows, rows), LOW),
        average=vmem((images, count, 128), WIDE), inverse=vmem((images, count, 128), WIDE),
        cols=vmem((2, count, 128), WIDE),
        w1_turned=vmem(w1.shape[::-1], LOW), w2_turned=vmem(w2.shape[::-1], LOW),
        logits=vmem((images, slots, count), WIDE), disp=vmem((images, slots, count), WIDE),
        comb=vmem((images, slots, count), WIDE), slot_in=vmem((images, slots, features), WIDE),
        stack=vmem((2 * pair * slots, features), LOW), found=vmem((2 * pair * slots, features), LOW),
        blk=vmem((chunks, experts, height, features), LOW),
        rows=vmem((chunks, spread, tensor, experts, height, features), LOW),
        s_all=vmem((total, features), LOW), g_all=vmem((total, features), LOW),
        h_all=vmem((total, units), LOW), p_all=vmem((total, units), LOW),
        pre=vmem((chunks * group if spread > 1 else group, units), WIDE),
        part=vmem((chunks, 2, group, features), WIDE),
        sent=vmem((chunks, 2, max(tensor - 1, 1), own, features), LOW),
        got=vmem((chunks, 2, max(tensor - 1, 1), own, features), LOW),
        ret=vmem((chunks, experts, height, features), LOW),
        back=vmem((chunks, experts, height, features), LOW),
        left=vmem((images, 4 * slots, count), LOW), right=vmem((images, slots, features), LOW),
        moment=vmem((images, 8, count), WIDE),
        keys_sum=vmem((slots, features), WIDE), gain_sum=vmem((slots, features), WIDE),
        pack=vmem((devices, each * 8, 128), WIDE),
        heap=vmem((devices, each * 8, 128), WIDE), total=vmem((each * 8, 128), WIDE),
        summed=vmem((devices, each * 8, 128), WIDE),
        in_sem=dma((4,)), image_sem=dma((2, images)), out_sem=dma((4,)), ends=dma((4,)),
        zs=dma((chunks,)), zr=dma((chunks, experts)), bs=dma((chunks,)), br=dma((chunks,)),
        ys=dma((chunks, max(tensor - 1, 1))), yr=dma((chunks, max(tensor - 1, 1))),
        xs=dma((chunks, tensor, max(spread - 1, 1))), xr=dma((chunks, tensor, max(spread - 1, 1))),
        ps=dma((chunks, 2, max(tensor - 1, 1))), pr=dma((chunks, 2, max(tensor - 1, 1))),
    )
    if finish:
        scratch.update(turned=vmem((features // dp, total), LOW))
    far, near = pl.BlockSpec(memory_space=pltpu.HBM), pl.BlockSpec(memory_space=vmem)
    names = list(ins) + list(outs) + list(scratch)
    values = pl.pallas_call(
        functools.partial(exchange_kernel, sizes, spread, finish, names),
        out_shape=[jax.ShapeDtypeStruct(shape, kind) for shape, kind in outs.values()],
        in_specs=[far] * len(ins),
        out_specs=[near] * held + [far] * (len(outs) - held),
        scratch_shapes=list(scratch.values()),
        compiler_params=pltpu.CompilerParams(
            collective_id=0, has_side_effects=True, vmem_limit_bytes=LIMIT if finish else LIMIT + LIMIT // 4
        ),
        name="exchange",
    )(*[pltpu.with_memory_space_constraint(v, pltpu.HBM) for v in ins.values()])
    return values[:held], values[held:]


def store_kernel(count, *refs):
    copies = [
        pltpu.make_async_copy(refs[n], refs[count + n], refs[-1].at[n]) for n in range(count)
    ]
    for copy in copies:
        copy.start()
    for copy in copies:
        copy.wait()


def store(values):
    count = len(values)
    return pl.pallas_call(
        functools.partial(store_kernel, count),
        out_shape=[jax.ShapeDtypeStruct(v.shape, v.dtype) for v in values],
        in_specs=[pl.BlockSpec(memory_space=pltpu.VMEM)] * count,
        out_specs=[pl.BlockSpec(memory_space=pltpu.HBM)] * count,
        scratch_shapes=[pltpu.SemaphoreType.DMA((count,))],
        compiler_params=pltpu.CompilerParams(vmem_limit_bytes=12 * 1024 * 1024),
        name="store",
    )(*values)


def local(sizes, tokens, cotangent, norm_gain, slot_keys, w_in, w_out):
    dp = sizes[0]
    features = tokens.shape[2]
    gain_rows, keys = norm_gain.reshape(features // 128, 128), slot_keys.T
    held, rows = exchange(sizes, tokens, cotangent, gain_rows, keys, w_in[0], w_out[0])
    grad_tokens, grad_gain, grad_keys, *rest = store(held)
    if rest:
        first_total, second_total = rest
    else:
        slot_rows, grad_rows, hidden, grad_pre = rows
        if dp > 2:
            slot_rows = lax.all_to_all(slot_rows, "dp", split_axis=1, concat_axis=0, tiled=True)
            grad_rows = lax.all_to_all(grad_rows, "dp", split_axis=1, concat_axis=0, tiled=True)
            hidden = lax.all_gather(hidden, "dp", axis=0, tiled=True)
            grad_pre = lax.all_gather(grad_pre, "dp", axis=0, tiled=True)
        else:
            width = features // dp
            start = lax.axis_index("dp") * width
            slot_rows = lax.dynamic_slice_in_dim(slot_rows, start, width, axis=1)
            grad_rows = lax.dynamic_slice_in_dim(grad_rows, start, width, axis=1)
        first_total = contract_rows(slot_rows, grad_pre).astype(LOW)
        second_total = contract_rows(hidden, grad_rows).astype(LOW)
    return (
        grad_tokens, grad_gain.reshape(features), grad_keys.T,
        first_total[None], second_total[None],
    )


def solution(mesh):
    tokens = P(("dp", "expert", "tensor"), None, None)
    return jax.shard_map(
        functools.partial(local, tuple(mesh.shape[name] for name in AXES)),
        mesh=mesh,
        in_specs=(tokens, tokens, P(), P(), P("expert", None, "tensor"), P("expert", "tensor", None)),
        out_specs=(tokens, P(), P(), P("expert", "dp", "tensor"), P("expert", "tensor", "dp")),
        check_vma=False,
    )
```

```python
import functools
import types

import jax
import jax.numpy as jnp
from jax import lax
from jax.experimental import pallas as pl
from jax.experimental.pallas import tpu as pltpu
from jax.sharding import PartitionSpec as P

AXES = ("dp", "expert", "tensor")
MESH = pl.DeviceIdType.MESH
SLOT_PER = 2
EPSILON = 1e-06
GELU_A = 0.7978845608028654
GELU_B = 0.044715
TILE = 256
ROWS = 64
LOW, WIDE = jnp.bfloat16, jnp.float32
LIMIT = 46 * 1024 * 1024


def contract_rows(left, right):
    return lax.dot_general(left, right, (((0,), (0,)), ((), ())), preferred_element_type=WIDE)


def contract_cols(left, right):
    return lax.dot_general(left, right, (((1,), (1,)), ((), ())), preferred_element_type=WIDE)


def gelu_of(x):
    return 0.5 * x * (1.0 + jnp.tanh(GELU_A * (x + GELU_B * (x * x * x))))


def gelu_slope(x):
    square = x * x
    bend = jnp.tanh(GELU_A * (x + GELU_B * (square * x)))
    return 0.5 * (1.0 + bend) + 0.5 * x * (1.0 - bend * bend) * (
        GELU_A * (1.0 + 3.0 * GELU_B * square)
    )


def around(position, step, size):
    return lax.rem(position + (step + size), size)


def orders(pair, experts, tensor):
    slots, quarter = experts * SLOT_PER, pair * SLOT_PER
    height, own = 2 * quarter, experts * quarter
    group = tensor * own

    def hot(size, source):
        row = lax.broadcasted_iota(jnp.int32, (size, size), 0)
        return (source(row) == lax.broadcasted_iota(jnp.int32, (size, size), 1)).astype(LOW)

    def image_order(r):
        e, stream, u = r // height, r % height // quarter, r % quarter
        return stream * (pair * slots) + u // SLOT_PER * slots + e * SLOT_PER + u % SLOT_PER

    def stream_order(r):
        e, stream, u = r // height, r % height // quarter, r % quarter
        return stream * own + e * quarter + u

    def block_order(r):
        return r % group // quarter * height + r // group * quarter + r % quarter

    def back_order(r):
        image, stream, slot = r // (2 * slots), r % (2 * slots) // slots, r % slots
        return slot // SLOT_PER * height + stream * quarter + image * SLOT_PER + slot % SLOT_PER

    rows = experts * height
    sizes = (rows, 2 * group, rows, rows)
    sources = (image_order, block_order, stream_order, back_order)
    return [functools.partial(hot, *pair) for pair in zip(sizes, sources)]


def exchange_kernel(sizes, spread, finish, names, *refs):
    dp, experts, tensor = sizes
    r = types.SimpleNamespace(**dict(zip(names, refs)))
    d, e, t = (lax.axis_index(name) for name in AXES)
    images, count, features = r.x.shape
    slots, units = r.keys.shape[0], r.w1.shape[1]
    chunks, _, height, _ = r.blk.shape
    pair, quarter = images // chunks, height // 2
    own = experts * quarter
    group = tensor * own
    lanes = features // 128
    mine = d if spread > 1 else 0
    where = [d, e, t]

    def push(src, dst, send, recv, axis, place):
        target = {"dp": d, "expert": e, "tensor": t}
        target[axis] = place
        return pltpu.make_async_remote_copy(
            src_ref=src, dst_ref=dst, send_sem=send, recv_sem=recv,
            device_id=tuple(target[name] for name in AXES), device_id_type=MESH,
        )

    def columns(tile, extent=features):
        return [slice(n, n + tile) for n in range(0, extent, tile)]

    offsets = [(a, b, c) for a in range(dp) for b in range(experts) for c in range(tensor)]
    targets = [tuple(around(w, k, s) for w, k, s in zip(where, step, sizes)) for step in offsets]
    sources = [tuple(around(w, -k, s) for w, k, s in zip(where, step, sizes)) for step in offsets]
    others = range(1, len(offsets))
    rank = lambda p: (p[0] * experts + p[1]) * tensor + p[2]

    fetched = []

    def fetch(src, dst):
        copy = pltpu.make_async_copy(src, dst, r.in_sem.at[len(fetched)])
        copy.start()
        fetched.append(copy)
        return copy

    def image_copy(b, n):
        some = b if b < pair else pl.ds(pair, images - pair)
        return pltpu.make_async_copy(
            (r.x_in, r.c_in)[n].at[some], (r.x, r.c)[n].at[some], r.image_sem.at[n, min(b, pair)])

    small = [fetch(r.gain_in, r.gain_rows), fetch(r.keys_in, r.keys)]
    for b in range(pair):
        image_copy(b, 0).start()
        image_copy(b, 1).start()
    barrier = pltpu.get_barrier_semaphore()
    for k in others:
        pl.semaphore_signal(barrier, inc=1, device_id=targets[k], device_id_type=MESH)
    if images > pair:
        image_copy(pair, 0).start()
        image_copy(pair, 1).start()
    w1_copy, w2_copy = fetch(r.w1_in, r.w1), fetch(r.w2_in, r.w2)
    image_order, block_order, stream_order, back_order = orders(pair, experts, tensor)
    r.keys_sum[...] = jnp.zeros_like(r.keys_sum)
    r.gain_sum[...] = jnp.zeros_like(r.gain_sum)

    def normalise(b):
        blocks = [slice(n, n + ROWS) for n in range(0, count, ROWS)]
        for rows in blocks:
            average = jnp.mean(r.x[b, rows, :].astype(WIDE), axis=-1, keepdims=True)
            r.average[b, rows, :] = jnp.broadcast_to(average, (ROWS, 128))
        for rows in blocks:
            average = r.average[b, rows, :]
            square = jnp.zeros((ROWS, 128), WIDE)
            for lane in columns(128):
                centred = r.x[b, rows, lane].astype(WIDE) - average
                square = square + centred * centred
            spread_of = jnp.sum(square, axis=-1, keepdims=True) * (1.0 / features)
            r.inverse[b, rows, :] = jnp.broadcast_to(lax.rsqrt(spread_of + EPSILON), (ROWS, 128))
        for rows in blocks:
            average, inverse = r.average[b, rows, :], r.inverse[b, rows, :]
            for n, lane in enumerate(columns(128)):
                centred = r.x[b, rows, lane].astype(WIDE) - average
                r.normed[b, rows, lane] = (centred * inverse * r.gain_rows[n:n + 1, :]).astype(LOW)

    def mix_image(b, slab):
        logits = contract_cols(r.keys[...], r.normed[b])
        over_tokens = jnp.exp(logits - jnp.max(logits, axis=1, keepdims=True))
        over_tokens = over_tokens / jnp.sum(over_tokens, axis=1, keepdims=True)
        over_slots = jnp.exp(logits - jnp.max(logits, axis=0, keepdims=True))
        over_slots = over_slots / jnp.sum(over_slots, axis=0, keepdims=True)
        r.logits[b] = logits
        r.disp[b] = over_tokens
        r.comb[b] = over_slots
        taken = jnp.dot(over_tokens.astype(LOW), r.normed[b], preferred_element_type=WIDE)
        given = jnp.dot(over_slots.astype(LOW), r.c[b], preferred_element_type=WIDE)
        r.slot_in[b] = taken
        r.stack[slab * slots:(slab + 1) * slots, :] = taken.astype(LOW)
        r.stack[(pair + slab) * slots:(pair + slab + 1) * slots, :] = given.astype(LOW)

    def pack_rows(c):
        moved = jnp.dot(r.mixes[...], r.stack[...], preferred_element_type=WIDE)
        for n in range(experts):
            r.blk[c, n] = moved[n * height:(n + 1) * height].astype(LOW)

    def partner(k):
        place = e
        for bit in (1 << n for n in range(k.bit_length()) if k >> n & 1):
            place = place + bit * (1 - 2 * lax.rem(lax.div(e, bit), 2))
        return place

    near = list(range(1, experts))
    if experts & (experts - 1) == 0:
        goes = comes = [partner(k) for k in range(experts)]
    else:
        goes = [around(e, k, experts) for k in range(experts)]
        comes = [around(e, -k, experts) for k in range(experts)]
    batch = max(experts // 4, 1)

    def scatter(c):
        share_rows(c, r.blk.at[c, e], 0)
        for k in near:
            push(r.blk.at[c, goes[k]], r.rows.at[c, mine, t, e],
                 r.zs.at[0], r.zr.at[c, k // batch], "expert", goes[k]).start()
        r.rows[c, mine, t, e] = r.blk[c, e]

    def share_rows(c, src, k):
        slot = r.rows.at[c, mine, t, comes[k]]
        for j in range(1, tensor):
            push(src, slot, r.ys.at[j - 1], r.yr.at[c, j - 1], "tensor", around(t, j, tensor)).start()

    def share_slab(c, j):
        for i in range(1, spread):
            slab = r.rows.at[c, mine, around(t, -j, tensor)]
            push(slab, slab, r.xs.at[i - 1], r.xr.at[i - 1], "dp", around(d, i, dp)).start()

    waiting = {}

    def forward_rows(c, upto=experts):
        ready = [k for k in waiting.setdefault(c, list(near)) if k < upto]
        for n in sorted({k // batch for k in ready}):
            some = [k for k in near if k // batch == n]
            slabs = r.rows.at[c, mine, t, pl.ds(0, len(some))]
            push(slabs, slabs, r.zs.at[0], r.zr.at[c, n], "expert", goes[1]).wait_recv()
            for k in some:
                waiting[c].remove(k)
                share_rows(c, r.rows.at[c, mine, t, comes[k]], k)
        if ready and not waiting[c]:
            share_slab(c, 0)

    def gather_rows(c):
        for j in range(1, tensor):
            slab = r.rows.at[c, mine, around(t, -j, tensor)]
            push(slab, slab, r.ys.at[j - 1], r.yr.at[c, j - 1], "tensor", around(t, j, tensor)).wait_recv()
            share_slab(c, j)

    def unpack(c, place, base):
        block = r.rows[c, place].reshape(2 * group, features)
        both = jnp.dot(r.unp[...], block, preferred_element_type=WIDE)
        r.s_all[base:base + group, :] = both[0:group].astype(LOW)
        r.g_all[base:base + group, :] = both[group:].astype(LOW)

    def transpose(weight, turned):
        row = lax.broadcasted_iota(jnp.int32, (TILE, TILE), 0)
        eye = (row == lax.broadcasted_iota(jnp.int32, (TILE, TILE), 1)).astype(LOW)

        @pl.loop(0, weight.shape[0] // TILE)
        def _(n):
            rows = pl.ds(pl.multiple_of(n * TILE, TILE), TILE)
            for cols in columns(TILE, weight.shape[1]):
                turned[cols, rows] = contract_cols(eye, weight[rows, cols]).astype(LOW)

    def forward(base, size):
        for cols in columns(TILE, units):
            x = jnp.dot(r.s_all[base:base + size, :], r.w1[:, cols], preferred_element_type=WIDE)
            r.pre[0:size, cols] = x
            r.h_all[base:base + size, cols] = gelu_of(x).astype(LOW)

    def backward(base, size):
        for cols in columns(TILE, units):
            x = jnp.dot(r.g_all[base:base + size, :], r.w2_turned[:, cols], preferred_element_type=WIDE)
            r.p_all[base:base + size, cols] = (x * gelu_slope(r.pre[0:size, cols])).astype(LOW)

    middle = -(-features // (2 * TILE)) * TILE
    whole = [slice(0, features)]
    halves = {c: whole for c in range(chunks)}
    if chunks > 2 and middle < features:
        halves[0] = halves[chunks - 1] = [slice(0, middle), slice(middle, features)]

    def tiles(span):
        return [slice(n, min(n + TILE, span.stop)) for n in range(span.start, span.stop, TILE)]

    def project(c, base, half=0):
        for cols in tiles(halves[c][half]):
            r.part[c, 0, :, cols] = jnp.dot(
                r.h_all[base:base + group, :], r.w2[:, cols], preferred_element_type=WIDE)
        share_part(c, 0, half)

    def project_back(c, base, half=0):
        for cols in tiles(halves[c][half]):
            r.part[c, 1, :, cols] = contract_cols(r.p_all[base:base + group, :], r.w1[cols, :])
        share_part(c, 1, half)

    def share_part(c, which, half):
        cols = halves[c][half]
        for j in range(1, tensor):
            to = around(t, j, tensor)
            r.sent[c, which, j - 1, :, cols] = r.part[
                c, which, pl.ds(pl.multiple_of(to * own, 8), own), cols].astype(LOW)
            push(r.sent.at[c, which, j - 1, :, cols], r.got.at[c, which, j - 1, :, cols],
                 r.ps.at[0], r.pr.at[c, half], "tensor", to).start()

    def give_back(c, half=0):
        cols = halves[c][half]
        totals = []
        if tensor > 1:
            both = r.got.at[c, :, :, :, cols]
            push(both, both, r.ps.at[0], r.pr.at[c, half], "tensor", around(t, 1, tensor)).wait_recv()
        for which in range(2):
            total = r.part[c, which, pl.ds(pl.multiple_of(t * own, 8), own), cols]
            for j in range(1, tensor):
                total = total + r.got[c, which, j - 1, :, cols].astype(WIDE)
            totals.append(total.astype(LOW))
        moved = jnp.dot(r.turn[...], jnp.concatenate(totals, axis=0), preferred_element_type=WIDE)
        for n in range(experts):
            r.ret[c, n, :, cols] = moved[n * height:(n + 1) * height].astype(LOW)
        for k in reversed(near):
            push(r.ret.at[c, goes[k], :, cols], r.back.at[c, e, :, cols],
                 r.bs.at[0], r.br.at[c, half], "expert", goes[k]).start()
        r.back[c, e, :, cols] = r.ret[c, e, :, cols]

    def image_gradients(b, slab):
        start = slab * 2 * slots
        returned = r.found[start:start + slots, :]
        slot_grad = r.found[start + slots:start + 2 * slots, :]
        grad_dispatch = contract_cols(slot_grad, r.normed[b])
        grad_combine = contract_cols(returned, r.c[b])
        dispatch, combine = r.disp[b], r.comb[b]
        logit = dispatch * (
            grad_dispatch - jnp.sum(dispatch * grad_dispatch, axis=1, keepdims=True)
        ) + combine * (grad_combine - jnp.sum(combine * grad_combine, axis=0, keepdims=True))
        first = logit.astype(LOW)
        rest = logit - first.astype(WIDE)
        second = rest.astype(LOW)
        third = (rest - second.astype(WIDE)).astype(LOW)
        low = dispatch.astype(LOW)
        split = jnp.concatenate([first, second, third], axis=0)
        r.left[b, 0:slots, :] = low
        r.left[b, slots:4 * slots, :] = split
        r.right[b] = slot_grad
        parts = jnp.dot(split, r.normed[b], preferred_element_type=WIDE)
        r.keys_sum[...] += parts[0:slots] + parts[slots:2 * slots] + parts[2 * slots:3 * slots]
        wide = slot_grad.astype(WIDE)
        r.gain_sum[...] += wide * r.slot_in[b]
        low = low.astype(WIDE)
        gains = r.gains[...]
        from_slots = jnp.sum(wide * gains, axis=1, keepdims=True)
        from_keys = jnp.sum(r.keys[...].astype(WIDE) * gains, axis=1, keepdims=True)
        first_mean = jnp.sum(low * from_slots + logit * from_keys, axis=0, keepdims=True)
        second_mean = jnp.sum(low * grad_dispatch + logit * r.logits[b], axis=0, keepdims=True)
        row = lax.broadcasted_iota(jnp.int32, (8, count), 0)
        r.moment[b] = jnp.where(row == 0, first_mean, second_mean) * (1.0 / features)

    def take_back(c):
        with jax.named_scope(f"waitback{c}"):
            for half, cols in enumerate(halves[c]):
                most = r.back.at[c, pl.ds(0, experts - 1), :, cols]
                push(most, most, r.bs.at[0], r.br.at[c, half], "expert", goes[1]).wait_recv()
        block = r.back[c].reshape(experts * height, features)
        r.found[...] = jnp.dot(r.sel[...], block, preferred_element_type=WIDE).astype(LOW)

        for slab in range(pair):
            image_gradients(c * pair + slab, slab)

    placed = []

    def place_out(src, dst):
        copy = pltpu.make_async_copy(src, dst, r.out_sem.at[len(placed)])
        copy.start()
        placed.append(copy)

    def finish_image(b):
        moment = r.moment[b].T
        average, inverse = r.average[b], r.inverse[b]
        first = jnp.broadcast_to(moment[:, 0:1], (count, 128))
        second = -inverse * inverse * moment[:, 1:2]
        r.cols[0] = first
        r.cols[1] = second
        left = r.left[b].T
        key = r.keys[...]
        for cols in columns(TILE):
            right = jnp.concatenate([r.right[b, :, cols]] + [key[:, cols]] * 3, axis=0)
            grads = jnp.dot(left, right, preferred_element_type=WIDE) * r.gains[:, cols]
            for n in range(0, TILE, 128):
                lane = slice(cols.start + n, cols.start + n + 128)
                scaled = (r.x[b, :, lane].astype(WIDE) - r.average[b]) * r.cols[1]
                change = r.inverse[b] * (grads[:, n:n + 128] - r.cols[0]) + scaled
                r.x[b, :, lane] = (r.c[b, :, lane].astype(WIDE) + change).astype(LOW)

    full = chunks * group

    def other_rows(i):
        other = around(d, -i, dp)
        slabs = r.rows.at[:, other]
        push(slabs, slabs, r.xs.at[i - 1], r.xr.at[i - 1], "dp", around(d, i, dp)).wait_recv()
        for c in range(chunks):
            unpack(c, other, i * full + c * group)

    scope = jax.named_scope

    def step(name, action):
        with scope(name):
            action()

    def weights_ready():
        w1_copy.wait()
        w2_copy.wait()

    def wait_image(b):
        if b <= pair:
            image_copy(b, 0).wait()
            image_copy(b, 1).wait()

    def set_gains():
        r.gains[...] = jnp.concatenate([r.gain_rows[n:n + 1, :] for n in range(lanes)], axis=1)

    def mix_pair(b, after):
        if after:
            wait_image(b + 1)
            normalise(b + 1)
        mix_image(b, b % pair)
        if b % pair == pair - 1:
            pack_rows(b // pair)

    def start_mix():
        r.mixes[...] = image_order()
        image_copy(0, 0).wait()
        for copy in small:
            copy.wait()
        normalise(0)

    def mix_first():
        image_copy(0, 1).wait()
        for b in range(1, pair):
            wait_image(b)
        for b in range(1, pair):
            normalise(b)
        for b in range(pair):
            mix_image(b, b)
        pack_rows(0)

    last = chunks - 1
    step("start", start_mix)
    quarters = [n * batch for n in range(1, experts // batch + 1)]
    step("mix01", mix_first)
    for b in range(pair - 1, images):
        c = b // pair
        if b >= pair:
            step(f"mix{b}", lambda: mix_pair(b, b + 1 < images))
        if b % pair == pair - 1:
            if c == 0:
                step("barrier", lambda: pl.semaphore_wait(barrier, len(others)))
            step(f"scatter{c}", lambda: scatter(c))
            if b == pair - 1 and images > pair:
                def more():
                    wait_image(b + 1)
                    normalise(b + 1)
                step("more", more)
        hook = b - pair
        if 0 <= hook < len(quarters) and images > pair:
            step(f"fwd0_{hook}", lambda: forward_rows(0, quarters[hook]))
    step("fwdrows0", lambda: forward_rows(0))
    if chunks > 1:
        step("fwd1_near", lambda: forward_rows(1, quarters[len(quarters) // 2 - 1]))
    r.unp[...], r.turn[...], r.sel[...] = block_order(), stream_order(), back_order()
    set_gains()
    step("weights", weights_ready)
    step("weights2", lambda: transpose(r.w2, r.w2_turned))
    if chunks > 1:
        step("fwdrows1", lambda: forward_rows(1))
    if chunks > 2:
        step("fwd2_near", lambda: forward_rows(2, quarters[len(quarters) // 2 - 1]))
    for c in range(chunks):
        base = c * group
        step(f"gather{c}", lambda: gather_rows(c))
        step(f"unpack{c}", lambda: unpack(c, mine, base))
        step(f"forward{c}", lambda: forward(base, group))
        if c > 1:
            step(f"giveback{c - 2}", lambda: give_back(c - 2, len(halves[c - 2]) - 1))
        step(f"project{c}", lambda: project(c, base))
        step(f"backward{c}", lambda: backward(base, group))
        if c == 1 and len(halves[0]) > 1:
            step("giveback0a", lambda: give_back(0))
        step(f"projback{c}", lambda: project_back(c, base))
        if c + 2 < chunks:
            step(f"fwdrows{c + 2}", lambda: forward_rows(c + 2))
        for half in range(1, len(halves[c])):
            step(f"project{c}", lambda: project(c, base, half))
            step(f"projback{c}", lambda: project_back(c, base, half))

    if finish:
        width = r.gin.shape[0]
        mine_cols = pl.ds(pl.multiple_of(d * width, 128), width)

    def add_up(i, total, out, place, value):
        if i > 0:
            value = value + total[place]
        if i == spread - 1:
            out[place] = value.astype(LOW)
        else:
            total[place] = value

    def product_in(i):
        rows = slice(i * full, (i + 1) * full)
        r.turned[...] = r.s_all[rows, mine_cols].T

        @pl.loop(0, units // TILE)
        def _(n):
            cols = pl.ds(pl.multiple_of(n * TILE, TILE), TILE)
            add_up(i, r.gin_sum, r.gin, (slice(None), cols), jnp.dot(
                r.turned[...], r.p_all[rows, cols], preferred_element_type=WIDE))

    def product_out():
        @pl.loop(0, units // TILE)
        def _(n):
            cols = pl.ds(pl.multiple_of(n * TILE, TILE), TILE)
            r.gout[cols, :] = contract_rows(r.h_all[:, cols], r.g_all[:, mine_cols]).astype(LOW)

    def other_forward():
        for i in range(1, spread):
            step("otherrows", lambda: other_rows(i))
            step("otherfwd", lambda: forward(i * full, full))

    for c in range(max(chunks - 2, 0), chunks):
        if finish and c == last:
            step("ownin", lambda: product_in(0))
        for half in range(len(halves[c])):
            step(f"giveback{c}_{half}", lambda: give_back(c, half))
    for c in range(last):
        step(f"takeback{c}", lambda: take_back(c))
        if c == 0:
            other_forward()
    if last == 0:
        other_forward()
    step(f"takeback{last}", lambda: take_back(last))

    each = r.pack.shape[1] // 8
    bands = slots // 8
    count_tiles = bands * lanes + -(-lanes // 8)
    owners = -(-count_tiles // each)
    me = rank(where)
    gain = jnp.sum(r.gain_sum[...] + r.keys[...].astype(WIDE) * r.keys_sum[...], axis=0, keepdims=True)
    gain = gain / r.gains[...]
    for n in range(bands * lanes):
        band, lane = n // lanes, n % lanes
        r.pack[n // each, pl.ds(n % each * 8, 8), :] = r.keys_sum[
            band * 8:band * 8 + 8, lane * 128:lane * 128 + 128]
    blank = jnp.zeros((1, 128), WIDE)
    for n in range(0, lanes, 8):
        m = bands * lanes + n // 8
        pieces = [gain[:, k * 128:k * 128 + 128] if k < lanes else blank for k in range(n, n + 8)]
        r.pack[m // each, m % each * 8:m % each * 8 + 8, :] = jnp.concatenate(pieces, axis=0)

    def reduce_copy(k):
        return pltpu.make_async_remote_copy(
            src_ref=r.pack.at[rank(targets[k])], dst_ref=r.heap.at[k], send_sem=r.ends.at[0],
            recv_sem=r.ends.at[1], device_id=targets[k], device_id_type=MESH)

    def spread_copy(k):
        return pltpu.make_async_remote_copy(
            src_ref=r.total, dst_ref=r.summed.at[me], send_sem=r.ends.at[2],
            recv_sem=r.ends.at[3], device_id=targets[k], device_id_type=MESH)

    def many(size, n):
        some = (r.heap if n == 0 else r.summed).at[pl.ds(0, size)]
        return pltpu.make_async_remote_copy(
            src_ref=some, dst_ref=some, send_sem=r.ends.at[n], recv_sem=r.ends.at[n + 1],
            device_id=targets[1], device_id_type=MESH)

    def gated(test, action):
        pl.when(test)(action)

    def by_owner(action):
        gated(me < owners, lambda: action(owners - 1))
        gated(me >= owners, lambda: action(owners))

    for k in others:
        gated(rank(targets[k]) < owners, lambda k=k: reduce_copy(k).start())

    def finish_images():
        @pl.loop(0, images)
        def _(b):
            finish_image(b)

    step("elem", finish_images)

    def reduce_own():
        @pl.when(me < owners)
        def _():
            r.heap[0] = r.pack[me]
            many(len(others), 0).wait_recv()
            r.total[...] = jnp.sum(r.heap[...], axis=0).astype(LOW)
            for k in others:
                spread_copy(k).start()
            r.summed[me] = r.total[...]

    step("reduceown", reduce_own)
    for i in range(1, spread):
        step("otherbwd", lambda: backward(i * full, full))
    if finish:
        for i in range(1, spread):
            step("productin", lambda: product_in(i))
        step("productout", product_out)
    else:
        place_out(r.s_all, r.s_out)
        place_out(r.g_all, r.g_out)
        place_out(r.h_all, r.h_out)
        place_out(r.p_all, r.p_out)

    def drain():
        def sent(src, semaphore):
            push(src, src, semaphore, r.zr.at[0, 0], "expert", goes[1]).wait_send()

        sent(r.rows.at[:, mine, t, pl.ds(0, experts - 1)], r.zs.at[0])
        sent(r.back.at[:, pl.ds(0, experts - 1)], r.bs.at[0])
        if tensor > 1:
            sent(r.got, r.ps.at[0])
        for j in range(1, tensor):
            sent(r.rows.at[:, mine, t], r.ys.at[j - 1])
        for i in range(1, spread):
            sent(r.rows.at[:, mine], r.xs.at[i - 1])
        by_owner(lambda size: many(size, 0).wait_send())

    step("drain", drain)

    def collect():
        by_owner(lambda size: many(size, 2).wait_recv())
        for n in range(bands * lanes):
            band, lane = n // lanes, n % lanes
            r.keys_out[band * 8:band * 8 + 8, lane * 128:lane * 128 + 128] = r.summed[
                n // each, n % each * 8:n % each * 8 + 8, :].astype(WIDE)
        for n in range(0, lanes, 8):
            m, some = bands * lanes + n // 8, min(8, lanes - n)
            whole = r.summed[m // each, m % each * 8:m % each * 8 + 8, :].astype(WIDE)
            r.gain_out[n:n + some, :] = whole[0:some]

        gated(me < owners, lambda: many(len(others), 2).wait_send())
        for copy in placed:
            copy.wait()

    step("collect", collect)


def exchange(sizes, tokens, cotangent, gain_rows, keys, w1, w2):
    dp, experts, tensor = sizes
    images, count, features = tokens.shape
    units = w1.shape[1]
    slots = experts * SLOT_PER
    pair = 2 if images % 2 == 0 else 1
    chunks = images // pair
    quarter = pair * SLOT_PER
    height = 2 * quarter
    own = experts * quarter
    group = tensor * own
    spread = dp if dp <= 2 else 1
    total = spread * chunks * group
    finish = spread == dp and features % (128 * dp) == 0
    devices = dp * experts * tensor
    lanes = features // 128
    count_tiles = slots // 8 * lanes + -(-lanes // 8)
    each = -(-count_tiles // devices)
    dma = pltpu.SemaphoreType.DMA
    vmem = pltpu.VMEM
    ins = dict(x_in=tokens, c_in=cotangent, gain_in=gain_rows, keys_in=keys, w1_in=w1, w2_in=w2)
    outs = dict(x=(tokens.shape, LOW), gain_out=(gain_rows.shape, WIDE), keys_out=(keys.shape, WIDE))
    if finish:
        outs.update(gin=((features // dp, units), LOW), gout=((units, features // dp), LOW))
    held = len(outs)
    if not finish:
        outs.update(s_out=((total, features), LOW), g_out=((total, features), LOW),
                    h_out=((total, units), LOW), p_out=((total, units), LOW))
    rows = experts * height
    scratch = dict(
        c=vmem(tokens.shape, LOW), normed=vmem(tokens.shape, LOW),
        gain_rows=vmem(gain_rows.shape, WIDE), gains=vmem((1, features), WIDE),
        keys=vmem(keys.shape, LOW), w1=vmem(w1.shape, LOW), w2=vmem(w2.shape, LOW),
        mixes=vmem((rows, rows), LOW), unp=vmem((2 * group, 2 * group), LOW),
        turn=vmem((rows, rows), LOW), sel=vmem((rows, rows), LOW),
        average=vmem((images, count, 128), WIDE), inverse=vmem((images, count, 128), WIDE),
        cols=vmem((2, count, 128), WIDE),
        w2_turned=vmem(w2.shape[::-1], LOW),
        logits=vmem((images, slots, count), WIDE), disp=vmem((images, slots, count), WIDE),
        comb=vmem((images, slots, count), WIDE), slot_in=vmem((images, slots, features), WIDE),
        stack=vmem((2 * pair * slots, features), LOW), found=vmem((2 * pair * slots, features), LOW),
        blk=vmem((chunks, experts, height, features), LOW),
        rows=vmem((chunks, spread, tensor, experts, height, features), LOW),
        s_all=vmem((total, features), LOW), g_all=vmem((total, features), LOW),
        h_all=vmem((total, units), LOW), p_all=vmem((total, units), LOW),
        pre=vmem((chunks * group if spread > 1 else group, units), WIDE),
        part=vmem((chunks, 2, group, features), WIDE),
        sent=vmem((chunks, 2, max(tensor - 1, 1), own, features), LOW),
        got=vmem((chunks, 2, max(tensor - 1, 1), own, features), LOW),
        ret=vmem((chunks, experts, height, features), LOW),
        back=vmem((chunks, experts, height, features), LOW),
        left=vmem((images, 4 * slots, count), LOW), right=vmem((images, slots, features), LOW),
        moment=vmem((images, 8, count), WIDE),
        keys_sum=vmem((slots, features), WIDE), gain_sum=vmem((slots, features), WIDE),
        pack=vmem((devices, each * 8, 128), WIDE),
        heap=vmem((devices, each * 8, 128), WIDE), total=vmem((each * 8, 128), LOW),
        summed=vmem((devices, each * 8, 128), LOW),
        in_sem=dma((4,)), image_sem=dma((2, pair + 1)), out_sem=dma((1 if finish else 4,)), ends=dma((4,)),
        zs=dma((1,)), zr=dma((chunks, experts // max(experts // 4, 1))), bs=dma((1,)), br=dma((chunks, 2)),
        ys=dma((max(tensor - 1, 1),)), yr=dma((chunks, max(tensor - 1, 1))),
        xs=dma((max(spread - 1, 1),)), xr=dma((max(spread - 1, 1),)),
        ps=dma((1,)), pr=dma((chunks, 2)),
    )
    if finish:
        scratch.update(turned=vmem((features // dp, total // spread), LOW),
                       gin_sum=vmem((features // dp, units), WIDE))
    far, near = pl.BlockSpec(memory_space=pltpu.HBM), pl.BlockSpec(memory_space=vmem)
    names = list(ins) + list(outs) + list(scratch)
    values = pl.pallas_call(
        functools.partial(exchange_kernel, sizes, spread, finish, names),
        out_shape=[jax.ShapeDtypeStruct(shape, kind) for shape, kind in outs.values()],
        in_specs=[far] * len(ins),
        out_specs=[near] * held + [far] * (len(outs) - held),
        scratch_shapes=list(scratch.values()),
        compiler_params=pltpu.CompilerParams(
            collective_id=0, has_side_effects=True, vmem_limit_bytes=LIMIT if finish else LIMIT + LIMIT // 8
        ),
        name="exchange",
    )(*[pltpu.with_memory_space_constraint(v, pltpu.HBM) for v in ins.values()])
    return values[:held], values[held:]


def store_kernel(count, *refs):
    copies = [
        pltpu.make_async_copy(refs[n], refs[count + n], refs[-1].at[n]) for n in range(count)
    ]
    for copy in copies:
        copy.start()
    for copy in copies:
        copy.wait()


def store(values):
    count = len(values)
    return pl.pallas_call(
        functools.partial(store_kernel, count),
        out_shape=[jax.ShapeDtypeStruct(v.shape, v.dtype) for v in values],
        in_specs=[pl.BlockSpec(memory_space=pltpu.VMEM)] * count,
        out_specs=[pl.BlockSpec(memory_space=pltpu.HBM)] * count,
        scratch_shapes=[pltpu.SemaphoreType.DMA((count,))],
        compiler_params=pltpu.CompilerParams(vmem_limit_bytes=12 * 1024 * 1024),
        name="store",
    )(*values)


def local(sizes, tokens, cotangent, norm_gain, slot_keys, w_in, w_out):
    dp = sizes[0]
    features = tokens.shape[2]
    gain_rows, keys = norm_gain.reshape(features // 128, 128), slot_keys.T
    held, rows = exchange(sizes, tokens, cotangent, gain_rows, keys, w_in[0], w_out[0])
    grad_tokens, grad_gain, grad_keys, *rest = store(held)
    if rest:
        first_total, second_total = rest
    else:
        slot_rows, grad_rows, hidden, grad_pre = rows
        if dp > 2:
            slot_rows = lax.all_to_all(slot_rows, "dp", split_axis=1, concat_axis=0, tiled=True)
            grad_rows = lax.all_to_all(grad_rows, "dp", split_axis=1, concat_axis=0, tiled=True)
            hidden = lax.all_gather(hidden, "dp", axis=0, tiled=True)
            grad_pre = lax.all_gather(grad_pre, "dp", axis=0, tiled=True)
        else:
            width = features // dp
            start = lax.axis_index("dp") * width
            slot_rows = lax.dynamic_slice_in_dim(slot_rows, start, width, axis=1)
            grad_rows = lax.dynamic_slice_in_dim(grad_rows, start, width, axis=1)
        first_total = contract_rows(slot_rows, grad_pre).astype(LOW)
        second_total = contract_rows(hidden, grad_rows).astype(LOW)
    return (
        grad_tokens, grad_gain.reshape(features), grad_keys.T,
        first_total[None], second_total[None],
    )


def solution(mesh):
    tokens = P(("dp", "expert", "tensor"), None, None)
    return jax.shard_map(
        functools.partial(local, tuple(mesh.shape[name] for name in AXES)),
        mesh=mesh,
        in_specs=(tokens, tokens, P(), P(), P("expert", None, "tensor"), P("expert", "tensor", None)),
        out_specs=(tokens, P(), P(), P("expert", "dp", "tensor"), P("expert", "tensor", "dp")),
        check_vma=False,
    )
```

```python
import functools
import types

import jax
import jax.numpy as jnp
import numpy as np
from jax import lax
from jax.experimental import pallas as pl
from jax.experimental.pallas import tpu as pltpu
from jax.sharding import PartitionSpec as P

AXES = ("dp", "expert", "tensor")
MESH = pl.DeviceIdType.MESH
SLOT_PER = 2
EPSILON = 1e-06
GELU_A = 0.7978845608028654
GELU_B = 0.044715
TILE = 256
ROWS = 64
LOW, WIDE = jnp.bfloat16, jnp.float32
LIMIT = 46 * 1024 * 1024


def contract_rows(left, right):
    return lax.dot_general(left, right, (((0,), (0,)), ((), ())), preferred_element_type=WIDE)


def contract_cols(left, right):
    return lax.dot_general(left, right, (((1,), (1,)), ((), ())), preferred_element_type=WIDE)


def gelu_of(x):
    return 0.5 * x * (1.0 + jnp.tanh(GELU_A * (x + GELU_B * (x * x * x))))


def gelu_slope(x):
    square = x * x
    bend = jnp.tanh(GELU_A * (x + GELU_B * (square * x)))
    return 0.5 * (1.0 + bend) + 0.5 * x * (1.0 - bend * bend) * (
        GELU_A * (1.0 + 3.0 * GELU_B * square)
    )


def around(position, step, size):
    return lax.rem(position + (step + size), size)


def orders(pair, experts, tensor):
    slots, quarter = experts * SLOT_PER, pair * SLOT_PER
    height, own = 2 * quarter, experts * quarter
    group = tensor * own

    def hot(size, source):
        row = lax.broadcasted_iota(jnp.int32, (size, size), 0)
        return (source(row) == lax.broadcasted_iota(jnp.int32, (size, size), 1)).astype(LOW)

    def image_order(r):
        e, stream, u = r // height, r % height // quarter, r % quarter
        return stream * (pair * slots) + u // SLOT_PER * slots + e * SLOT_PER + u % SLOT_PER

    def stream_order(r):
        e, stream, u = r // height, r % height // quarter, r % quarter
        return stream * own + e * quarter + u

    def block_order(r):
        return r % group // quarter * height + r // group * quarter + r % quarter

    def back_order(r):
        image, stream, slot = r // (2 * slots), r % (2 * slots) // slots, r % slots
        return slot // SLOT_PER * height + stream * quarter + image * SLOT_PER + slot % SLOT_PER

    rows = experts * height
    sizes = (rows, 2 * group, rows, rows)
    sources = (image_order, block_order, stream_order, back_order)
    return [functools.partial(hot, *pair) for pair in zip(sizes, sources)]


def exchange_kernel(sizes, spread, finish, names, *refs):
    dp, experts, tensor = sizes
    r = types.SimpleNamespace(**dict(zip(names, refs)))
    d, e, t = (lax.axis_index(name) for name in AXES)
    images, count, features = r.x.shape
    slots, units = r.keys.shape[0], r.w1.shape[1]
    chunks, _, height, _ = r.blk.shape
    pair, quarter = images // chunks, height // 2
    own = experts * quarter
    group = tensor * own
    lanes = features // 128
    mine = d if spread > 1 else 0
    where = [d, e, t]

    def push(src, dst, send, recv, axis, place):
        target = {"dp": d, "expert": e, "tensor": t}
        target[axis] = place
        return pltpu.make_async_remote_copy(
            src_ref=src, dst_ref=dst, send_sem=send, recv_sem=recv,
            device_id=tuple(target[name] for name in AXES), device_id_type=MESH,
        )

    def columns(tile, extent=features):
        return [slice(n, n + tile) for n in range(0, extent, tile)]

    offsets = [(a, b, c) for a in range(dp) for b in range(experts) for c in range(tensor)]
    targets = [tuple(around(w, k, s) for w, k, s in zip(where, step, sizes)) for step in offsets]
    sources = [tuple(around(w, -k, s) for w, k, s in zip(where, step, sizes)) for step in offsets]
    others = range(1, len(offsets))
    rank = lambda p: (p[0] * experts + p[1]) * tensor + p[2]

    fetched = []

    def fetch(src, dst):
        copy = pltpu.make_async_copy(src, dst, r.in_sem.at[len(fetched)])
        copy.start()
        fetched.append(copy)
        return copy

    def image_copy(b, n):
        some = b if b < pair else pl.ds(pair, images - pair)
        return pltpu.make_async_copy(
            (r.x_in, r.c_in)[n].at[some], (r.x, r.c)[n].at[some], r.image_sem.at[n, min(b, pair)])

    small = [fetch(r.gain_in, r.gain_rows), fetch(r.keys_in, r.keys)]
    for b in range(pair):
        image_copy(b, 0).start()
        image_copy(b, 1).start()
    barrier = pltpu.get_barrier_semaphore()
    for k in others:
        pl.semaphore_signal(barrier, inc=1, device_id=targets[k], device_id_type=MESH)
    if images > pair:
        image_copy(pair, 0).start()
        image_copy(pair, 1).start()
    w1_copy, w2_copy = fetch(r.w1_in, r.w1), fetch(r.w2_in, r.w2)
    image_order, block_order, stream_order, back_order = orders(pair, experts, tensor)
    r.keys_sum[...] = jnp.zeros_like(r.keys_sum)
    r.gain_sum[...] = jnp.zeros_like(r.gain_sum)

    def normalise(b):
        blocks = [slice(n, n + ROWS) for n in range(0, count, ROWS)]
        for rows in blocks:
            average = jnp.mean(r.x[b, rows, :].astype(WIDE), axis=-1, keepdims=True)
            r.average[b, rows, :] = jnp.broadcast_to(average, (ROWS, 128))
        for rows in blocks:
            average = r.average[b, rows, :]
            square = jnp.zeros((ROWS, 128), WIDE)
            for lane in columns(128):
                centred = r.x[b, rows, lane].astype(WIDE) - average
                square = square + centred * centred
            spread_of = jnp.sum(square, axis=-1, keepdims=True) * (1.0 / features)
            r.inverse[b, rows, :] = jnp.broadcast_to(lax.rsqrt(spread_of + EPSILON), (ROWS, 128))
        for rows in blocks:
            average, inverse = r.average[b, rows, :], r.inverse[b, rows, :]
            for n, lane in enumerate(columns(128)):
                centred = r.x[b, rows, lane].astype(WIDE) - average
                r.normed[b, rows, lane] = (centred * inverse * r.gain_rows[n:n + 1, :]).astype(LOW)

    def mix_image(b, slab):
        logits = contract_cols(r.keys[...], r.normed[b])
        over_tokens = jnp.exp(logits - jnp.max(logits, axis=1, keepdims=True))
        over_tokens = over_tokens / jnp.sum(over_tokens, axis=1, keepdims=True)
        over_slots = jnp.exp(logits - jnp.max(logits, axis=0, keepdims=True))
        over_slots = over_slots / jnp.sum(over_slots, axis=0, keepdims=True)
        r.logits[b] = logits
        r.disp[b] = over_tokens
        r.comb[b] = over_slots
        taken = jnp.dot(over_tokens.astype(LOW), r.normed[b], preferred_element_type=WIDE)
        given = jnp.dot(over_slots.astype(LOW), r.c[b], preferred_element_type=WIDE)
        r.slot_in[b] = taken
        r.stack[slab * slots:(slab + 1) * slots, :] = taken.astype(LOW)
        r.stack[(pair + slab) * slots:(pair + slab + 1) * slots, :] = given.astype(LOW)

    def pack_rows(c):
        moved = jnp.dot(r.mixes[...], r.stack[...], preferred_element_type=WIDE)
        for n in range(experts):
            r.blk[c, n] = moved[n * height:(n + 1) * height].astype(LOW)

    def partner(k):
        place = e
        for bit in (1 << n for n in range(k.bit_length()) if k >> n & 1):
            place = place + bit * (1 - 2 * lax.rem(lax.div(e, bit), 2))
        return place

    near = list(range(1, experts))
    if experts & (experts - 1) == 0:
        goes = comes = [partner(k) for k in range(experts)]
    else:
        goes = [around(e, k, experts) for k in range(experts)]
        comes = [around(e, -k, experts) for k in range(experts)]
    batch = max(experts // 4, 1)

    def scatter(c):
        share_rows(c, r.blk.at[c, e], 0)
        for k in near:
            push(r.blk.at[c, goes[k]], r.rows.at[c, mine, t, e],
                 r.zs.at[0], r.zr.at[c, k // batch], "expert", goes[k]).start()
        r.rows[c, mine, t, e] = r.blk[c, e]

    def share_rows(c, src, k):
        slot = r.rows.at[c, mine, t, comes[k]]
        for j in range(1, tensor):
            push(src, slot, r.ys.at[j - 1], r.yr.at[c, j - 1], "tensor", around(t, j, tensor)).start()

    def share_slab(c, j):
        for i in range(1, spread):
            slab = r.rows.at[c, mine, around(t, -j, tensor)]
            push(slab, slab, r.xs.at[i - 1], r.xr.at[i - 1], "dp", around(d, i, dp)).start()

    waiting = {}

    def forward_rows(c, upto=experts):
        ready = [k for k in waiting.setdefault(c, list(near)) if k < upto]
        for n in sorted({k // batch for k in ready}):
            some = [k for k in near if k // batch == n]
            slabs = r.rows.at[c, mine, t, pl.ds(0, len(some))]
            push(slabs, slabs, r.zs.at[0], r.zr.at[c, n], "expert", goes[1]).wait_recv()
            for k in some:
                waiting[c].remove(k)
                share_rows(c, r.rows.at[c, mine, t, comes[k]], k)
        if ready and not waiting[c]:
            share_slab(c, 0)

    def gather_rows(c):
        for j in range(1, tensor):
            slab = r.rows.at[c, mine, around(t, -j, tensor)]
            push(slab, slab, r.ys.at[j - 1], r.yr.at[c, j - 1], "tensor", around(t, j, tensor)).wait_recv()
            share_slab(c, j)

    def unpack(c, place, base):
        block = r.rows[c, place].reshape(2 * group, features)
        both = jnp.dot(r.unp[...], block, preferred_element_type=WIDE)
        r.s_all[base:base + group, :] = both[0:group].astype(LOW)
        r.g_all[base:base + group, :] = both[group:].astype(LOW)

    def transpose(weight, turned):
        row = lax.broadcasted_iota(jnp.int32, (TILE, TILE), 0)
        eye = (row == lax.broadcasted_iota(jnp.int32, (TILE, TILE), 1)).astype(LOW)

        @pl.loop(0, weight.shape[0] // TILE)
        def _(n):
            rows = pl.ds(pl.multiple_of(n * TILE, TILE), TILE)
            for cols in columns(TILE, weight.shape[1]):
                turned[cols, rows] = contract_cols(eye, weight[rows, cols]).astype(LOW)

    def forward(base, size):
        for cols in columns(TILE, units):
            x = jnp.dot(r.s_all[base:base + size, :], r.w1[:, cols], preferred_element_type=WIDE)
            r.pre[0:size, cols] = x
            r.h_all[base:base + size, cols] = gelu_of(x).astype(LOW)

    def backward(base, size):
        for cols in columns(TILE, units):
            x = jnp.dot(r.g_all[base:base + size, :], r.w2_turned[:, cols], preferred_element_type=WIDE)
            r.p_all[base:base + size, cols] = (x * gelu_slope(r.pre[0:size, cols])).astype(LOW)

    middle = -(-features // (2 * TILE)) * TILE
    whole = [slice(0, features)]
    halves = {c: whole for c in range(chunks)}
    if chunks > 2 and middle < features:
        halves[0] = halves[chunks - 1] = [slice(0, middle), slice(middle, features)]

    def tiles(span):
        return [slice(n, min(n + TILE, span.stop)) for n in range(span.start, span.stop, TILE)]

    def project(c, base, half=0):
        for cols in tiles(halves[c][half]):
            r.part[c, 0, :, cols] = jnp.dot(
                r.h_all[base:base + group, :], r.w2[:, cols], preferred_element_type=WIDE)
        share_part(c, 0, half)

    def project_back(c, base, half=0):
        for cols in tiles(halves[c][half]):
            r.part[c, 1, :, cols] = contract_cols(r.p_all[base:base + group, :], r.w1[cols, :])
        share_part(c, 1, half)

    def share_part(c, which, half):
        cols = halves[c][half]
        for j in range(1, tensor):
            to = around(t, j, tensor)
            r.sent[c, which, j - 1, :, cols] = r.part[
                c, which, pl.ds(pl.multiple_of(to * own, 8), own), cols].astype(LOW)
            push(r.sent.at[c, which, j - 1, :, cols], r.got.at[c, which, j - 1, :, cols],
                 r.ps.at[0], r.pr.at[c, half], "tensor", to).start()

    def give_back(c, half=0):
        cols = halves[c][half]
        totals = []
        if tensor > 1:
            both = r.got.at[c, :, :, :, cols]
            push(both, both, r.ps.at[0], r.pr.at[c, half], "tensor", around(t, 1, tensor)).wait_recv()
        for which in range(2):
            total = r.part[c, which, pl.ds(pl.multiple_of(t * own, 8), own), cols]
            for j in range(1, tensor):
                total = total + r.got[c, which, j - 1, :, cols].astype(WIDE)
            totals.append(total.astype(LOW))
        moved = jnp.dot(r.turn[...], jnp.concatenate(totals, axis=0), preferred_element_type=WIDE)
        for n in range(experts):
            r.ret[c, n, :, cols] = moved[n * height:(n + 1) * height].astype(LOW)
        for k in reversed(near):
            push(r.ret.at[c, goes[k], :, cols], r.back.at[c, e, :, cols],
                 r.bs.at[0], r.br.at[c, half], "expert", goes[k]).start()
        r.back[c, e, :, cols] = r.ret[c, e, :, cols]

    def image_gradients(b, slab):
        start = slab * 2 * slots
        returned = r.found[start:start + slots, :]
        slot_grad = r.found[start + slots:start + 2 * slots, :]
        grad_dispatch = contract_cols(slot_grad, r.normed[b])
        grad_combine = contract_cols(returned, r.c[b])
        dispatch, combine = r.disp[b], r.comb[b]
        logit = dispatch * (
            grad_dispatch - jnp.sum(dispatch * grad_dispatch, axis=1, keepdims=True)
        ) + combine * (grad_combine - jnp.sum(combine * grad_combine, axis=0, keepdims=True))
        first = logit.astype(LOW)
        rest = logit - first.astype(WIDE)
        second = rest.astype(LOW)
        third = (rest - second.astype(WIDE)).astype(LOW)
        low = dispatch.astype(LOW)
        split = jnp.concatenate([first, second, third], axis=0)
        r.left[b, 0:slots, :] = low
        r.left[b, slots:4 * slots, :] = split
        r.right[b] = slot_grad
        parts = jnp.dot(split, r.normed[b], preferred_element_type=WIDE)
        r.keys_sum[...] += parts[0:slots] + parts[slots:2 * slots] + parts[2 * slots:3 * slots]
        wide = slot_grad.astype(WIDE)
        r.gain_sum[...] += wide * r.slot_in[b]
        low = low.astype(WIDE)
        gains = r.gains[...]
        from_slots = jnp.sum(wide * gains, axis=1, keepdims=True)
        from_keys = jnp.sum(r.keys[...].astype(WIDE) * gains, axis=1, keepdims=True)
        first_mean = jnp.sum(low * from_slots + logit * from_keys, axis=0, keepdims=True)
        second_mean = jnp.sum(low * grad_dispatch + logit * r.logits[b], axis=0, keepdims=True)
        row = lax.broadcasted_iota(jnp.int32, (8, count), 0)
        r.moment[b] = jnp.where(row == 0, first_mean, second_mean) * (1.0 / features)

    def take_back(c):
        with jax.named_scope(f"waitback{c}"):
            for half, cols in enumerate(halves[c]):
                most = r.back.at[c, pl.ds(0, experts - 1), :, cols]
                push(most, most, r.bs.at[0], r.br.at[c, half], "expert", goes[1]).wait_recv()
        block = r.back[c].reshape(experts * height, features)
        r.found[...] = jnp.dot(r.sel[...], block, preferred_element_type=WIDE).astype(LOW)

        for slab in range(pair):
            image_gradients(c * pair + slab, slab)

    placed = []

    def place_out(src, dst):
        copy = pltpu.make_async_copy(src, dst, r.out_sem.at[len(placed)])
        copy.start()
        placed.append(copy)

    def finish_image(b):
        moment = r.moment[b].T
        average, inverse = r.average[b], r.inverse[b]
        first = jnp.broadcast_to(moment[:, 0:1], (count, 128))
        second = -inverse * inverse * moment[:, 1:2]
        r.cols[0] = first
        r.cols[1] = second
        left = r.left[b].T
        key = r.keys[...]
        for cols in columns(TILE):
            right = jnp.concatenate([r.right[b, :, cols]] + [key[:, cols]] * 3, axis=0)
            grads = jnp.dot(left, right, preferred_element_type=WIDE) * r.gains[:, cols]
            for n in range(0, TILE, 128):
                lane = slice(cols.start + n, cols.start + n + 128)
                scaled = (r.x[b, :, lane].astype(WIDE) - r.average[b]) * r.cols[1]
                change = r.inverse[b] * (grads[:, n:n + 128] - r.cols[0]) + scaled
                r.x[b, :, lane] = (r.c[b, :, lane].astype(WIDE) + change).astype(LOW)

    full = chunks * group

    def other_rows(i):
        other = around(d, -i, dp)
        slabs = r.rows.at[:, other]
        push(slabs, slabs, r.xs.at[i - 1], r.xr.at[i - 1], "dp", around(d, i, dp)).wait_recv()
        for c in range(chunks):
            unpack(c, other, i * full + c * group)

    scope = jax.named_scope

    def step(name, action):
        with scope(name):
            action()

    def weights_ready():
        w1_copy.wait()
        w2_copy.wait()

    def wait_image(b):
        if b <= pair:
            image_copy(b, 0).wait()
            image_copy(b, 1).wait()

    def set_gains():
        r.gains[...] = jnp.concatenate([r.gain_rows[n:n + 1, :] for n in range(lanes)], axis=1)

    def mix_pair(b, after):
        if after:
            wait_image(b + 1)
            normalise(b + 1)
        mix_image(b, b % pair)
        if b % pair == pair - 1:
            pack_rows(b // pair)

    def start_mix():
        r.mixes[...] = image_order()
        image_copy(0, 0).wait()
        for copy in small:
            copy.wait()
        normalise(0)

    def mix_first():
        image_copy(0, 1).wait()
        for b in range(1, pair):
            wait_image(b)
        for b in range(1, pair):
            normalise(b)
        for b in range(pair):
            mix_image(b, b)
        pack_rows(0)

    last = chunks - 1
    step("start", start_mix)
    quarters = [n * batch for n in range(1, experts // batch + 1)]
    step("mix01", mix_first)
    for b in range(pair - 1, images):
        c = b // pair
        if b >= pair:
            step(f"mix{b}", lambda: mix_pair(b, b + 1 < images))
        if b % pair == pair - 1:
            if c == 0:
                step("barrier", lambda: pl.semaphore_wait(barrier, len(others)))
            step(f"scatter{c}", lambda: scatter(c))
            if b == pair - 1 and images > pair:
                def more():
                    wait_image(b + 1)
                    normalise(b + 1)
                step("more", more)
        hook = b - pair
        if 0 <= hook < len(quarters) and images > pair:
            step(f"fwd0_{hook}", lambda: forward_rows(0, quarters[hook]))
    step("fwdrows0", lambda: forward_rows(0))
    if chunks > 1:
        step("fwd1_near", lambda: forward_rows(1, quarters[len(quarters) // 2 - 1]))
    r.unp[...], r.turn[...], r.sel[...] = block_order(), stream_order(), back_order()
    set_gains()
    step("weights", weights_ready)
    step("weights2", lambda: transpose(r.w2, r.w2_turned))
    if chunks > 1:
        step("fwdrows1", lambda: forward_rows(1))
    if chunks > 2:
        step("fwd2_near", lambda: forward_rows(2, quarters[len(quarters) // 2 - 1]))
    for c in range(chunks):
        base = c * group
        step(f"gather{c}", lambda: gather_rows(c))
        step(f"unpack{c}", lambda: unpack(c, mine, base))
        step(f"forward{c}", lambda: forward(base, group))
        if c > 1:
            step(f"giveback{c - 2}", lambda: give_back(c - 2, len(halves[c - 2]) - 1))
        step(f"project{c}", lambda: project(c, base))
        step(f"backward{c}", lambda: backward(base, group))
        if c == 1 and len(halves[0]) > 1:
            step("giveback0a", lambda: give_back(0))
        step(f"projback{c}", lambda: project_back(c, base))
        if c + 2 < chunks:
            step(f"fwdrows{c + 2}", lambda: forward_rows(c + 2))
        for half in range(1, len(halves[c])):
            step(f"project{c}", lambda: project(c, base, half))
            step(f"projback{c}", lambda: project_back(c, base, half))

    if finish:
        width = r.gin.shape[0]
        mine_cols = pl.ds(pl.multiple_of(d * width, 128), width)

    def add_up(i, total, out, place, value):
        if i > 0:
            value = value + total[place]
        if i == spread - 1:
            out[place] = value.astype(LOW)
        else:
            total[place] = value

    def product_in(i):
        rows = slice(i * full, (i + 1) * full)
        r.turned[...] = r.s_all[rows, mine_cols].T

        @pl.loop(0, units // TILE)
        def _(n):
            cols = pl.ds(pl.multiple_of(n * TILE, TILE), TILE)
            add_up(i, r.gin_sum, r.gin, (slice(None), cols), jnp.dot(
                r.turned[...], r.p_all[rows, cols], preferred_element_type=WIDE))

    def product_out():
        @pl.loop(0, units // TILE)
        def _(n):
            cols = pl.ds(pl.multiple_of(n * TILE, TILE), TILE)
            r.gout[cols, :] = contract_rows(r.h_all[:, cols], r.g_all[:, mine_cols]).astype(LOW)

    def other_forward():
        for i in range(1, spread):
            step("otherrows", lambda: other_rows(i))
            step("otherfwd", lambda: forward(i * full, full))

    for c in range(max(chunks - 2, 0), chunks):
        if finish and c == last:
            step("ownin", lambda: product_in(0))
        for half in range(len(halves[c])):
            step(f"giveback{c}_{half}", lambda: give_back(c, half))
    for c in range(last):
        step(f"takeback{c}", lambda: take_back(c))
        if c == 0:
            other_forward()
    if last == 0:
        other_forward()
    step(f"takeback{last}", lambda: take_back(last))

    each = r.pack.shape[1] // 8
    bands = slots // 8
    count_tiles = bands * lanes + -(-lanes // 8)
    owners = -(-count_tiles // each)
    me = rank(where)
    gain = jnp.sum(r.gain_sum[...] + r.keys[...].astype(WIDE) * r.keys_sum[...], axis=0, keepdims=True)
    gain = gain / r.gains[...]
    for n in range(bands * lanes):
        band, lane = n // lanes, n % lanes
        r.pack[n // each, pl.ds(n % each * 8, 8), :] = r.keys_sum[
            band * 8:band * 8 + 8, lane * 128:lane * 128 + 128]
    blank = jnp.zeros((1, 128), WIDE)
    for n in range(0, lanes, 8):
        m = bands * lanes + n // 8
        pieces = [gain[:, k * 128:k * 128 + 128] if k < lanes else blank for k in range(n, n + 8)]
        r.pack[m // each, m % each * 8:m % each * 8 + 8, :] = jnp.concatenate(pieces, axis=0)

    def reduce_copy(k):
        return pltpu.make_async_remote_copy(
            src_ref=r.pack.at[rank(targets[k])], dst_ref=r.heap.at[k], send_sem=r.ends.at[0],
            recv_sem=r.ends.at[1], device_id=targets[k], device_id_type=MESH)

    def spread_copy(k):
        return pltpu.make_async_remote_copy(
            src_ref=r.total, dst_ref=r.summed.at[me], send_sem=r.ends.at[2],
            recv_sem=r.ends.at[3], device_id=targets[k], device_id_type=MESH)

    def many(size, n):
        some = (r.heap if n == 0 else r.summed).at[pl.ds(0, size)]
        return pltpu.make_async_remote_copy(
            src_ref=some, dst_ref=some, send_sem=r.ends.at[n], recv_sem=r.ends.at[n + 1],
            device_id=targets[1], device_id_type=MESH)

    def gated(test, action):
        pl.when(test)(action)

    def by_owner(action):
        gated(me < owners, lambda: action(owners - 1))
        gated(me >= owners, lambda: action(owners))

    for k in others:
        gated(rank(targets[k]) < owners, lambda k=k: reduce_copy(k).start())

    def finish_images():
        @pl.loop(0, images)
        def _(b):
            finish_image(b)

    step("elem", finish_images)

    def reduce_own():
        @pl.when(me < owners)
        def _():
            r.heap[0] = r.pack[me]
            many(len(others), 0).wait_recv()
            r.total[...] = jnp.sum(r.heap[...], axis=0).astype(LOW)
            for k in others:
                spread_copy(k).start()
            r.summed[me] = r.total[...]

    step("reduceown", reduce_own)
    for i in range(1, spread):
        step("otherbwd", lambda: backward(i * full, full))
    if finish:
        for i in range(1, spread):
            step("productin", lambda: product_in(i))
        step("productout", product_out)
    else:
        place_out(r.s_all, r.s_out)
        place_out(r.g_all, r.g_out)
        place_out(r.h_all, r.h_out)
        place_out(r.p_all, r.p_out)

    def drain():
        def sent(src, semaphore):
            push(src, src, semaphore, r.zr.at[0, 0], "expert", goes[1]).wait_send()

        sent(r.rows.at[:, mine, t, pl.ds(0, experts - 1)], r.zs.at[0])
        sent(r.back.at[:, pl.ds(0, experts - 1)], r.bs.at[0])
        if tensor > 1:
            sent(r.got, r.ps.at[0])
        for j in range(1, tensor):
            sent(r.rows.at[:, mine, t], r.ys.at[j - 1])
        for i in range(1, spread):
            sent(r.rows.at[:, mine], r.xs.at[i - 1])
        by_owner(lambda size: many(size, 0).wait_send())

    step("drain", drain)

    def collect():
        by_owner(lambda size: many(size, 2).wait_recv())
        for n in range(bands * lanes):
            band, lane = n // lanes, n % lanes
            r.keys_out[band * 8:band * 8 + 8, lane * 128:lane * 128 + 128] = r.summed[
                n // each, n % each * 8:n % each * 8 + 8, :].astype(WIDE)
        for n in range(0, lanes, 8):
            m, some = bands * lanes + n // 8, min(8, lanes - n)
            whole = r.summed[m // each, m % each * 8:m % each * 8 + 8, :].astype(WIDE)
            r.gain_out[n:n + some, :] = whole[0:some]

        gated(me < owners, lambda: many(len(others), 2).wait_send())
        for copy in placed:
            copy.wait()

    step("collect", collect)


def exchange(sizes, tokens, cotangent, gain_rows, keys, w1, w2):
    dp, experts, tensor = sizes
    images, count, features = tokens.shape
    units = w1.shape[1]
    slots = experts * SLOT_PER
    pair = 2 if images % 2 == 0 else 1
    chunks = images // pair
    quarter = pair * SLOT_PER
    height = 2 * quarter
    own = experts * quarter
    group = tensor * own
    spread = dp if dp <= 2 else 1
    total = spread * chunks * group
    finish = spread == dp and features % (128 * dp) == 0
    devices = dp * experts * tensor
    lanes = features // 128
    count_tiles = slots // 8 * lanes + -(-lanes // 8)
    each = -(-count_tiles // devices)
    dma = pltpu.SemaphoreType.DMA
    vmem = pltpu.VMEM
    ins = dict(x_in=tokens, c_in=cotangent, gain_in=gain_rows, keys_in=keys, w1_in=w1, w2_in=w2)
    outs = dict(x=(tokens.shape, LOW), gain_out=(gain_rows.shape, WIDE), keys_out=(keys.shape, WIDE))
    if finish:
        outs.update(gin=((features // dp, units), LOW), gout=((units, features // dp), LOW))
    held = len(outs)
    if not finish:
        outs.update(s_out=((total, features), LOW), g_out=((total, features), LOW),
                    h_out=((total, units), LOW), p_out=((total, units), LOW))
    rows = experts * height
    scratch = dict(
        c=vmem(tokens.shape, LOW), normed=vmem(tokens.shape, LOW),
        gain_rows=vmem(gain_rows.shape, WIDE), gains=vmem((1, features), WIDE),
        keys=vmem(keys.shape, LOW), w1=vmem(w1.shape, LOW), w2=vmem(w2.shape, LOW),
        mixes=vmem((rows, rows), LOW), unp=vmem((2 * group, 2 * group), LOW),
        turn=vmem((rows, rows), LOW), sel=vmem((rows, rows), LOW),
        average=vmem((images, count, 128), WIDE), inverse=vmem((images, count, 128), WIDE),
        cols=vmem((2, count, 128), WIDE),
        w2_turned=vmem(w2.shape[::-1], LOW),
        logits=vmem((images, slots, count), WIDE), disp=vmem((images, slots, count), WIDE),
        comb=vmem((images, slots, count), WIDE), slot_in=vmem((images, slots, features), WIDE),
        stack=vmem((2 * pair * slots, features), LOW), found=vmem((2 * pair * slots, features), LOW),
        blk=vmem((chunks, experts, height, features), LOW),
        rows=vmem((chunks, spread, tensor, experts, height, features), LOW),
        s_all=vmem((total, features), LOW), g_all=vmem((total, features), LOW),
        h_all=vmem((total, units), LOW), p_all=vmem((total, units), LOW),
        pre=vmem((chunks * group if spread > 1 else group, units), WIDE),
        part=vmem((chunks, 2, group, features), WIDE),
        sent=vmem((chunks, 2, max(tensor - 1, 1), own, features), LOW),
        got=vmem((chunks, 2, max(tensor - 1, 1), own, features), LOW),
        ret=vmem((chunks, experts, height, features), LOW),
        back=vmem((chunks, experts, height, features), LOW),
        left=vmem((images, 4 * slots, count), LOW), right=vmem((images, slots, features), LOW),
        moment=vmem((images, 8, count), WIDE),
        keys_sum=vmem((slots, features), WIDE), gain_sum=vmem((slots, features), WIDE),
        pack=vmem((devices, each * 8, 128), WIDE),
        heap=vmem((devices, each * 8, 128), WIDE), total=vmem((each * 8, 128), LOW),
        summed=vmem((devices, each * 8, 128), LOW),
        in_sem=dma((4,)), image_sem=dma((2, pair + 1)), out_sem=dma((1 if finish else 4,)), ends=dma((4,)),
        zs=dma((1,)), zr=dma((chunks, experts // max(experts // 4, 1))), bs=dma((1,)), br=dma((chunks, 2)),
        ys=dma((max(tensor - 1, 1),)), yr=dma((chunks, max(tensor - 1, 1))),
        xs=dma((max(spread - 1, 1),)), xr=dma((max(spread - 1, 1),)),
        ps=dma((1,)), pr=dma((chunks, 2)),
    )
    if finish:
        scratch.update(turned=vmem((features // dp, total // spread), LOW),
                       gin_sum=vmem((features // dp, units), WIDE))
    far, near = pl.BlockSpec(memory_space=pltpu.HBM), pl.BlockSpec(memory_space=vmem)
    names = list(ins) + list(outs) + list(scratch)
    values = pl.pallas_call(
        functools.partial(exchange_kernel, sizes, spread, finish, names),
        out_shape=[jax.ShapeDtypeStruct(shape, kind) for shape, kind in outs.values()],
        in_specs=[far] * len(ins),
        out_specs=[near] * held + [far] * (len(outs) - held),
        scratch_shapes=list(scratch.values()),
        compiler_params=pltpu.CompilerParams(
            collective_id=0, has_side_effects=True, vmem_limit_bytes=LIMIT if finish else LIMIT + LIMIT // 8
        ),
        name="exchange",
    )(*[pltpu.with_memory_space_constraint(v, pltpu.HBM) for v in ins.values()])
    return values[:held], values[held:]


def store_kernel(count, *refs):
    copies = [
        pltpu.make_async_copy(refs[n], refs[count + n], refs[-1].at[n]) for n in range(count)
    ]
    order = sorted(range(count), key=lambda n: -np.prod(refs[n].shape))
    for n in order:
        size = refs[n].shape[0]
        parts = size if len(refs[n].shape) == 3 else 4 if size % 32 == 0 else 1
        for m in range(parts):
            some = pl.ds(m * (size // parts), size // parts)
            pltpu.make_async_copy(
                refs[n].at[some], refs[count + n].at[some], refs[-1].at[n]).start()
    for copy in copies:
        copy.wait()


def store(values):
    count = len(values)
    return pl.pallas_call(
        functools.partial(store_kernel, count),
        out_shape=[jax.ShapeDtypeStruct(v.shape, v.dtype) for v in values],
        in_specs=[pl.BlockSpec(memory_space=pltpu.VMEM)] * count,
        out_specs=[pl.BlockSpec(memory_space=pltpu.HBM)] * count,
        scratch_shapes=[pltpu.SemaphoreType.DMA((count,))],
        compiler_params=pltpu.CompilerParams(vmem_limit_bytes=12 * 1024 * 1024),
        name="store",
    )(*values)


def local(sizes, tokens, cotangent, norm_gain, slot_keys, w_in, w_out):
    dp = sizes[0]
    features = tokens.shape[2]
    gain_rows, keys = norm_gain.reshape(features // 128, 128), slot_keys.T
    held, rows = exchange(sizes, tokens, cotangent, gain_rows, keys, w_in[0], w_out[0])
    grad_tokens, grad_gain, grad_keys, *rest = store(held)
    if rest:
        first_total, second_total = rest
    else:
        slot_rows, grad_rows, hidden, grad_pre = rows
        if dp > 2:
            slot_rows = lax.all_to_all(slot_rows, "dp", split_axis=1, concat_axis=0, tiled=True)
            grad_rows = lax.all_to_all(grad_rows, "dp", split_axis=1, concat_axis=0, tiled=True)
            hidden = lax.all_gather(hidden, "dp", axis=0, tiled=True)
            grad_pre = lax.all_gather(grad_pre, "dp", axis=0, tiled=True)
        else:
            width = features // dp
            start = lax.axis_index("dp") * width
            slot_rows = lax.dynamic_slice_in_dim(slot_rows, start, width, axis=1)
            grad_rows = lax.dynamic_slice_in_dim(grad_rows, start, width, axis=1)
        first_total = contract_rows(slot_rows, grad_pre).astype(LOW)
        second_total = contract_rows(hidden, grad_rows).astype(LOW)
    return (
        grad_tokens, grad_gain.reshape(features), grad_keys.T,
        first_total[None], second_total[None],
    )


def solution(mesh):
    tokens = P(("dp", "expert", "tensor"), None, None)
    return jax.shard_map(
        functools.partial(local, tuple(mesh.shape[name] for name in AXES)),
        mesh=mesh,
        in_specs=(tokens, tokens, P(), P(), P("expert", None, "tensor"), P("expert", "tensor", None)),
        out_specs=(tokens, P(), P(), P("expert", "dp", "tensor"), P("expert", "tensor", "dp")),
        check_vma=False,
    )
```
